32 devices in a mesh: band: 4 (over y, core), col: 8 (over z, x).
Axes of the slice: x: 2, y: 2, z: 4, core: 2. Of those that a mesh axis runs over, the one named last changes fastest.
Arguments:
- source: bfloat16 [6, 524288], P(None, ('band', 'col')), may hold values from -6 to 6
- weights: bfloat16 [8192, 128, 128], P(('band', 'col')), may hold values from -0.5 to 0.5
- source_block: int32 [8192], P(('band', 'col')), may hold values from 0 to 127
- owner_device: int32 [8192, 1], P(('band', 'col')), may hold values from 0 to 31, as said below
- target_tile: int32 [8192], P(('band', 'col')), may hold values from 0 to 112, as said below
- cutoff: int32 [64], P(('band', 'col')), may hold values from 1 to 511
Outputs:
- remapped: float32 [6, 64, 7200], P(None, 'band', 'col')
- filtered: float32 [6, 64, 7200], P(None, 'band', 'col')
The draws below stay inside these ranges and needn't reach their ends.
Inputs may be any that keep to these rules, and one draw needn't show every extreme that they name: `owner_device`: owners are numbered band index times 8 plus col index. A device's blocks go only to owners in its own band or in the bands next to it. Among the 256 blocks of one device at most 24 share an owner; in every device exactly 24 do for some owner of its own band, and exactly 24 for some owner of each band next to its own; every device sends at least 15 blocks to each owner of its own band. `target_tile`: every tile of every owner receives at least one block.
All inputs are finite; a program needn't handle non-finite values.
Results may differ from the reference program's by a relative error of at most 0.0003.
Values sent between devices are 32-bit elements; how exact they have to be, the bound alone decides.
A program may use at most 64 MiB of HBM per device.

```python
import jax
import jax.numpy as jnp
from jax import lax

NLON = 7200
BLK = 128
LEV = 6
KW = 512
NB = 256
SB = 128
LATB = 16
NLAT = 64
LON_DEV = 900
TILES_DEV = 113
REG = 15
CAP = 24
NBLOCKS = 8192
NSRC = 524288
N_BAND = 4
N_COL = 8
DEVICES = 32


def remap_layout(key):
    slot_total = 3 * N_COL * CAP
    slots = jnp.arange(slot_total, dtype=jnp.int32)
    offset = slots // (N_COL * CAP)
    owner_col = slots // CAP % N_COL
    within = slots % CAP
    shifts = jax.random.randint(jax.random.fold_in(key, 11), (DEVICES,), 0, TILES_DEV).astype(jnp.int32)

    def one_device(device):
        device_key = jax.random.fold_in(jax.random.fold_in(key, 17), device)
        band = device // N_COL
        column = device % N_COL
        owner_band = band + offset - 1
        valid = (owner_band >= 0) & (owner_band < N_BAND)
        regular = (offset == 1) & (within < REG)
        candidate = valid & ((offset != 1) | (within >= REG))
        forced_cols = jax.random.randint(jax.random.fold_in(device_key, 1), (3,), 0, N_COL).astype(jnp.int32)
        forced = candidate & (owner_col == forced_cols[offset])
        ranking = jax.random.permutation(jax.random.fold_in(device_key, 2), slot_total).astype(jnp.int32)
        score = jnp.where(regular, 0, jnp.where(forced, 1, jnp.where(candidate, 2 + ranking, 4 * slot_total + 4)))
        chosen = jnp.argsort(score, stable=True)[:NB].astype(jnp.int32)
        mixing = jax.random.permutation(jax.random.fold_in(device_key, 3), NB).astype(jnp.int32)
        chosen = chosen[mixing]
        owners = (owner_band[chosen] * N_COL + owner_col[chosen]).astype(jnp.int32)
        random_tile = jax.random.randint(jax.random.fold_in(device_key, 4), (NB,), 0, TILES_DEV).astype(jnp.int32)
        regular_tile = (column * REG + within[chosen] + shifts[owners]) % TILES_DEV
        tiles = jnp.where(regular[chosen], regular_tile, random_tile).astype(jnp.int32)
        return (owners, tiles)
    owners, tiles = jax.vmap(one_device)(jnp.arange(DEVICES, dtype=jnp.int32))
    return (owners.reshape(NBLOCKS, 1).astype(jnp.int32), tiles.reshape(NBLOCKS).astype(jnp.int32))


def draw_owner_device(key, part):
    return remap_layout(jax.random.fold_in(key, 5))[0]


def draw_target_tile(key, part):
    return remap_layout(jax.random.fold_in(key, 5))[1]


def place_ends(array, key, low, high):
    place = [jax.random.randint(jax.random.fold_in(key, axis), (), 0, length) for axis, length in enumerate(array.shape)]
    longest = array.shape.index(max(array.shape))
    beside = place[:longest] + [(place[longest] + 1) % array.shape[longest]] + place[longest + 1:]
    return array.at[tuple(place)].set(low).at[tuple(beside)].set(high)


def levels(rng, dims, pieces, low, largest):
    factor_of, own = 1.0, jax.random.fold_in(rng, 6)
    for position, parts in pieces:
        draws = jnp.exp(jax.random.uniform(jax.random.fold_in(own, position), (parts,), jnp.float32, low / len(pieces), largest / len(pieces)))
        factor_of = factor_of * jnp.repeat(draws, dims[position] // parts).reshape([-1 if axis == position else 1 for axis in range(len(dims))])
    return factor_of


def centred(own_key, dims, width, most, split=(), kind=jnp.bfloat16):
    gain = levels(own_key, dims, split, -0.22, 0.18) if split else 1.0
    result = jax.random.normal(own_key, dims, jnp.float32) * width * gain
    return jnp.minimum(jnp.maximum(result, -most), most).astype(kind)


def setup_inputs(seed: int = 0) -> dict:
    splits = jax.random.split(jax.random.key(seed), 7)
    source = centred(splits[0], (LEV, NSRC), 1.0, 6.0, ((1, 32),))
    weights = centred(splits[1], (NBLOCKS, BLK, BLK), BLK ** -0.5, 0.5, ((0, 32),))
    source_block = place_ends(jax.random.randint(splits[2], (NBLOCKS,), 0, SB), jax.random.fold_in(splits[2], 1), 0, SB - 1).astype(jnp.int32)
    owner_device = draw_owner_device(jax.random.fold_in(splits[6], 71), 0)
    target_tile = draw_target_tile(jax.random.fold_in(splits[6], 71), 0)
    cutoff = place_ends(jax.random.randint(splits[5], (NLAT,), 1, KW), jax.random.fold_in(splits[5], 1), 1, KW - 1).astype(jnp.int32)
    return {"source": source, "weights": weights, "source_block": source_block, "owner_device": owner_device, "target_tile": target_tile, "cutoff": cutoff}


TWO_PI = 6.283185307179586


def zonal_table(start_index, length, period, wave_count):
    positions = start_index + lax.broadcasted_iota(jnp.int32, (length, wave_count), 0)
    wave_index = lax.broadcasted_iota(jnp.int32, (length, wave_count), 1)
    phases = (positions * wave_index) % period
    angles = phases.astype(jnp.float32) * (TWO_PI / period)
    return jnp.concatenate([jnp.cos(angles), jnp.sin(angles)], axis=1)


def spectral_weights(cutoffs, wave_count, period):
    wave_index = lax.broadcasted_iota(jnp.int32, (cutoffs.shape[0], wave_count), 1)
    scaled = jnp.where(wave_index == 0, 1.0, 2.0) / period
    retained = jnp.where(wave_index <= cutoffs[:, None], scaled, 0.0).astype(jnp.float32)
    return jnp.concatenate([retained, retained], axis=1)


def reference(source, weights, source_block, owner_device, target_tile, cutoff):
    device_total = N_BAND * N_COL
    blocks_all = source.reshape(LEV, device_total * SB, BLK)
    owners_all = owner_device[:, 0]

    def add_device(totals, device_index):
        first_block = device_index * NB
        block_weights = lax.dynamic_slice_in_dim(weights, first_block, NB, 0)
        chosen = lax.dynamic_slice_in_dim(source_block, first_block, NB, 0)
        owners = lax.dynamic_slice_in_dim(owners_all, first_block, NB, 0)
        tiles_hit = lax.dynamic_slice_in_dim(target_tile, first_block, NB, 0)
        picked = jnp.take(blocks_all, (device_index * SB + chosen).astype(jnp.int32), axis=1)
        partial_value = jnp.einsum("lnb,nbt->nlt", picked.astype(jnp.float32), block_weights.astype(jnp.float32))
        totals = totals.at[(owners * TILES_DEV + tiles_hit).astype(jnp.int32)].add(partial_value)
        return totals, None

    totals, unused = lax.scan(add_device, jnp.zeros((device_total * TILES_DEV, LEV, BLK), jnp.float32), jnp.arange(device_total, dtype=jnp.int32))
    cell_count = LATB * LON_DEV
    tiles = totals.reshape(N_BAND, N_COL, TILES_DEV, LEV, BLK)
    tiles = jnp.transpose(tiles, (3, 0, 1, 2, 4)).reshape(LEV, N_BAND, N_COL, TILES_DEV * BLK)[:, :, :, :cell_count]
    tiles = tiles.reshape(LEV, N_BAND, N_COL, LATB, LON_DEV)
    remapped = jnp.transpose(tiles, (0, 1, 3, 2, 4)).reshape(LEV, NLAT, NLON)
    wave_table = zonal_table(0, NLON, NLON, KW)
    spectrum = jnp.dot(remapped.reshape(LEV * NLAT, NLON), wave_table, precision=lax.Precision.HIGHEST, preferred_element_type=jnp.float32)
    spectrum = spectrum.reshape(LEV, NLAT, 2 * KW) * spectral_weights(cutoff, KW, NLON)[None]
    filtered = jnp.dot(spectrum.reshape(LEV * NLAT, 2 * KW), wave_table.T, precision=lax.Precision.HIGHEST, preferred_element_type=jnp.float32)
    return remapped, filtered.reshape(LEV, NLAT, NLON)
```

```python
import functools

import jax
import jax.numpy as jnp
import numpy as np
from jax import lax
from jax.experimental import pallas as pl
from jax.experimental.pallas import tpu as pltpu
from jax.sharding import PartitionSpec as P

NLON = 7200
KW = 512
LANES = 128
STEP = 16
CHUNK = 32
PIECE = 8
MESH = pl.DeviceIdType.MESH
F32 = jnp.float32
BF16 = jnp.bfloat16


def round_up(value, multiple):
    return (value + multiple - 1) // multiple * multiple


def split(value):
    high = value.astype(BF16)
    return high, (value - high.astype(F32)).astype(BF16)


def dot(left, right, left_dim=1, right_dim=0):
    return lax.dot_general(
        left, right, (((left_dim,), (right_dim,)), ((), ())), preferred_element_type=F32
    )


def remap_kernel(
    bands, cols, levels, capacity, wave_count, period, longitudes, tile_count,
    cutoff, source_block, owner_row, tile_row, fine, coarse, start, source, weights,
    remapped, filtered,
    weight_buf, source_buf, source_even, source_odd, partial,
    sums, table_high, table_low, rotated, field, slab, recv, relay, relay_sums, passed,
    tags_out, tags_in, cut_out, cut_in,
    spectra, arrived, half_sum, other_sum, scaled, gathered,
    weight_sem, source_sem, tag_send, tag_recv, cut_send, cut_recv,
    send_sem, recv_sem, relay_sem, pass_send, pass_recv,
    scatter_send, scatter_recv, cross_send, cross_recv, spread_send, spread_recv,
):
    band, col = lax.axis_index("band"), lax.axis_index("col")
    blocks = weights.shape[0]
    rows = levels * capacity
    half_size = cols // 2
    half, place_in_half = col // half_size, lax.rem(col, half_size)
    counterpart = (band, (1 - half) * half_size + place_in_half)

    def valid(offset):
        target = band + (offset - 1)
        return (target >= 0) & (target < bands)

    weight_copies = [
        pltpu.make_async_copy(
            weights.at[pl.ds(first, CHUNK)], weight_buf.at[pl.ds(first, CHUNK)], weight_sem.at[i]
        )
        for i, first in enumerate(range(0, blocks, CHUNK))
    ]
    source_copy = pltpu.make_async_copy(source, source_buf, source_sem)
    source_copy.start()
    for copy in weight_copies:
        copy.start()

    barrier = pltpu.get_barrier_semaphore()

    def greet(device):
        pl.semaphore_signal(barrier, inc=1, device_id=device, device_id_type=MESH)

    def greet_half(offset):
        def one(to, carry):
            def signal():
                greet((band + (offset - 1), half * half_size + to))

            if offset == 1:
                pl.when(to != place_in_half)(signal)
            else:
                signal()
            return carry

        lax.fori_loop(0, half_size, one, 0)

    for offset in (0, 2, 1):
        pl.when(valid(offset))(functools.partial(greet_half, offset))
    greet(counterpart)

    owners = owner_row[...]
    sublane = lax.broadcasted_iota(jnp.int32, (blocks, blocks), 0)
    lane = lax.broadcasted_iota(jnp.int32, (blocks, blocks), 1)
    owners_wide = jnp.broadcast_to(owners.astype(F32), (8, blocks))
    owner_column = jnp.transpose(owners_wide)[:, 0:1]
    earlier = (owner_column == owners.astype(F32)) & (sublane < lane)
    rank = jnp.sum(earlier.astype(jnp.int32), axis=0, keepdims=True)
    place = owners - (band - 1) * cols
    slot = place * capacity + rank
    slot_lane = lax.broadcasted_iota(jnp.int32, (LANES, blocks), 0)
    tile_at = jnp.where(slot_lane == rank, tile_row[...], 0).astype(F32).astype(BF16)
    place_ids = lax.broadcasted_iota(jnp.int32, (3 * cols, blocks), 0)
    chosen = (place_ids == place).astype(F32).astype(BF16)
    tags = dot(chosen, tile_at, 1, 1)
    for offset in range(3):
        for to in range(half_size):
            first = tags[offset * cols + to : offset * cols + to + 1]
            second = tags[offset * cols + half_size + to : offset * cols + half_size + to + 1]
            tags_out[offset * half_size + to, 0:1] = jnp.where(half == 0, first, second)
            tags_out[offset * half_size + to, 1:2] = jnp.where(half == 0, second, first)
    lat_here = cutoff.shape[0]
    for lat in range(lat_here):
        cut_out[lat : lat + 1] = jnp.full((1, LANES), cutoff[lat], jnp.int32)

    source_copy.wait()
    above = jnp.zeros((16 - levels, LANES), BF16)
    below = jnp.zeros((8, LANES), BF16)
    for index in range(source_even.shape[0]):
        value = source_buf[:, index * LANES : (index + 1) * LANES]
        source_even[index] = jnp.concatenate([value, above], axis=0)
        source_odd[index] = jnp.concatenate([below, value, above[: 8 - levels]], axis=0)

    for i, copy in enumerate(weight_copies):
        copy.wait()
        for index in range(i * CHUNK, (i + 1) * CHUNK, 2):
            left = jnp.concatenate(
                [source_even[source_block[index]], source_odd[source_block[index + 1]]], axis=1
            )
            right = weight_buf[index : index + 2].reshape(2 * LANES, LANES)
            partial[index : index + 2] = dot(left, right).reshape(2, 8, LANES)

    inner_band = (band > 0) & (band < bands - 1)
    neighbours = jnp.where(inner_band, 2, 1) if bands > 1 else 0
    pl.semaphore_wait(barrier, half_size * (1 + neighbours))

    def send_to_half(source_of, target, sems_out, sems_in, offset):
        def one(step, carry):
            to = lax.rem(place_in_half + half_size // 2 + step, half_size)

            def start_remote():
                pltpu.make_async_remote_copy(
                    src_ref=source_of(to),
                    dst_ref=target,
                    send_sem=sems_out.at[offset],
                    recv_sem=sems_in.at[2 - offset],
                    device_id=(band + (offset - 1), half * half_size + to),
                    device_id_type=MESH,
                ).start()

            if offset == 1:
                pl.when(to != place_in_half)(start_remote)
            else:
                start_remote()
            return carry

        lax.fori_loop(0, half_size, one, 0)
        if offset == 1:
            pltpu.make_async_copy(source_of(place_in_half), target, sems_in.at[1]).start()

    def push_tags(offset):
        send_to_half(
            lambda to: tags_out.at[offset * half_size + to],
            tags_in.at[(2 - offset) * half_size + place_in_half],
            tag_send, tag_recv, offset,
        )

    def push(owner_half, into, sems, offset):
        send_to_half(
            lambda to: slab.at[offset * cols + owner_half * half_size + to],
            into.at[(2 - offset) * half_size + place_in_half],
            send_sem, sems, offset,
        )

    cut_copy = pltpu.make_async_remote_copy(
        src_ref=cut_out,
        dst_ref=cut_in,
        send_sem=cut_send,
        recv_sem=cut_recv,
        device_id=counterpart,
        device_id_type=MESH,
    )
    for offset in (0, 2, 1):
        pl.when(valid(offset))(functools.partial(push_tags, offset))
    cut_copy.start()

    data = jnp.concatenate([partial[:, level, :] for level in range(levels)], axis=1)
    stacked = jnp.concatenate(split(data), axis=0)

    def fill(offset):
        group = cols * capacity
        ids = lax.broadcasted_iota(jnp.int32, (group, blocks), 0) + offset * group
        placing = (ids == slot).astype(F32).astype(BF16)
        placed = dot(jnp.concatenate([placing, placing], axis=1), stacked)
        here = pl.ds(offset * cols, cols)
        for level in range(levels):
            piece = placed[:, level * LANES : (level + 1) * LANES]
            slab[here, level * capacity : (level + 1) * capacity, :] = piece.reshape(
                cols, capacity, LANES
            )

    def place_and_push(offset):
        fill(offset)
        push(1 - half, relay, relay_sem, offset)

    for offset in (0, 2, 1):
        pl.when(valid(offset))(functools.partial(place_and_push, offset))
    for offset in (0, 2, 1):
        pl.when(valid(offset))(functools.partial(push, half, recv, recv_sem, offset))

    begin = start[col]
    cos_start, sin_start = begin[0:1], begin[1:2]
    rotated[0] = fine[0] * cos_start - fine[1] * sin_start
    rotated[1] = fine[1] * cos_start + fine[0] * sin_start
    parity = wave_count // 2

    def table_step(step, carry):
        pair = coarse[step]
        cos_base, sin_base = pair[0:1], pair[1:2]
        cos_fine, sin_fine = rotated[0], rotated[1]
        at = pl.ds(pl.multiple_of(step * STEP, STEP), STEP)
        for first, value in (
            (0, cos_base * cos_fine - sin_base * sin_fine),
            (parity, sin_base * cos_fine + cos_base * sin_fine),
        ):
            high, low = split(value)
            for odd in range(2):
                here = slice(first + odd * wave_count, first + odd * wave_count + parity)
                there = slice(odd * parity, (odd + 1) * parity)
                table_high[at, here] = high[:, there]
                table_low[at, here] = low[:, there]
        return carry

    lax.fori_loop(0, coarse.shape[0], table_step, 0)

    tiles = sums.shape[1]
    sums[...] = jnp.zeros_like(sums)
    relay_sums[...] = jnp.zeros_like(relay_sums)

    def wait_tags(offset):
        here = tags_in.at[pl.ds(offset * half_size, half_size)]
        pltpu.make_async_copy(here, here, tag_recv.at[offset]).wait()

    for offset in (0, 2, 1):
        pl.when(valid(offset))(functools.partial(wait_tags, offset))

    def receive(ref, sems, into, kind, offset):
        here = pl.ds(offset * half_size, half_size)
        tag_rows = [
            tags_in[offset * half_size + sender, kind : kind + 1] for sender in range(half_size)
        ]
        tags = jnp.transpose(jnp.concatenate(tag_rows * (-(-8 // half_size)), axis=0))
        wide = lax.broadcasted_iota(jnp.int32, (capacity, tiles), 1).astype(F32)
        chooser = jnp.concatenate(
            [
                (tags[:capacity, sender : sender + 1] == wide).astype(F32)
                for sender in range(half_size)
            ],
            axis=0,
        )
        chooser = jnp.transpose(chooser).astype(BF16)
        pltpu.make_async_copy(ref.at[here], ref.at[here], sems.at[offset]).wait()
        incoming = jnp.concatenate(
            [
                ref[here, level * capacity : (level + 1) * capacity, :].reshape(
                    half_size * capacity, LANES
                )
                for level in range(levels)
            ],
            axis=1,
        )
        high, low = split(incoming)
        total = dot(chooser, high) + dot(chooser, low)
        for level in range(levels):
            into[level] += total[:, level * LANES : (level + 1) * LANES]

    def dense_start(first, count):
        here = (pl.ds(first, count), pl.ds(0, tile_count))
        pltpu.make_async_remote_copy(
            src_ref=relay_sums.at[here],
            dst_ref=passed.at[pl.ds(first, count)],
            send_sem=pass_send,
            recv_sem=pass_recv,
            device_id=counterpart,
            device_id_type=MESH,
        ).start()

    outer = (place_in_half < half_size // 2) == (half == 0)
    inner = jnp.logical_not(outer)
    first_part, second_part = levels // 4, levels // 2

    for offset in (0, 2, 1):
        pl.when(valid(offset))(functools.partial(receive, relay, relay_sem, relay_sums, 1, offset))
    pl.when(inner)(functools.partial(dense_start, 0, levels))
    for offset in (0, 2, 1):
        pl.when(valid(offset))(functools.partial(receive, recv, recv_sem, sums, 0, offset))

    long_tiles, field_rows = field.shape[1:3]
    lat_band = field_rows // levels
    group_rows = field_rows // half_size
    shape3 = (levels, long_tiles, LANES)
    lane3 = lax.broadcasted_iota(jnp.int32, shape3, 2)
    inside = lax.broadcasted_iota(jnp.int32, shape3, 1) * LANES + lane3 < longitudes

    def row_of(level, lat):
        owner, within = divmod(lat, lat_here)
        lat_half, owner_place = divmod(owner, half_size)
        return owner_place * group_rows + (level * 2 + lat_half) * lat_here + within

    def lat_rows(ref, lat):
        first, shift = divmod(lat * longitudes, LANES)
        value = ref[:, first : first + long_tiles, :]
        if shift:
            after = ref[:, first + 1 : first + 1 + long_tiles, :]
            value = jnp.where(
                lane3 < LANES - shift,
                pltpu.roll(value, LANES - shift, 2),
                pltpu.roll(after, LANES - shift, 2),
            )
        return jnp.where(inside, value, 0.0)

    for lat in range(lat_band):
        own, relayed = lat_rows(sums, lat), lat_rows(relay_sums, lat)
        both, apart = own + relayed, own - relayed
        for level in range(levels):
            field[0, :, row_of(level, lat), :] = both[level]
            field[1, :, row_of(level, lat), :] = apart[level]

    for odd in range(2):
        rows_wide = jnp.concatenate([field[odd, tile] for tile in range(long_tiles)], axis=1)
        high, low = split(rows_wide)
        waves = slice(odd * wave_count, (odd + 1) * wave_count)
        both = dot(jnp.concatenate([high, low], axis=0), table_high[:, waves])
        spectrum = both[:field_rows] + both[field_rows:] + dot(high, table_low[:, waves])
        spectra[:, :, waves] = spectrum.reshape(half_size, group_rows, wave_count)

    pieces = [pl.ds(first, PIECE) for first in range(0, group_rows, PIECE)]

    def to_half(source_of, target, sem_out, sem_in):
        def one(step, carry):
            to = lax.rem(place_in_half + half_size // 2 + step, half_size)

            def start_remote():
                pltpu.make_async_remote_copy(
                    src_ref=source_of(to),
                    dst_ref=target,
                    send_sem=sem_out,
                    recv_sem=sem_in,
                    device_id=(band, half * half_size + to),
                    device_id_type=MESH,
                ).start()

            pl.when(to != place_in_half)(start_remote)
            return carry

        lax.fori_loop(0, half_size, one, 0)
        pltpu.make_async_copy(source_of(place_in_half), target, sem_in).start()

    for i, piece in enumerate(pieces):
        to_half(
            lambda to: spectra.at[to, piece],
            arrived.at[place_in_half, piece],
            scatter_send.at[i], scatter_recv.at[i],
        )
    pl.when(outer)(functools.partial(dense_start, 0, first_part))

    cut_copy.wait()
    cuts = []
    for lat_half in range(2):
        for lat in range(lat_here):
            cuts.append(
                jnp.where(half == lat_half, cut_out[lat : lat + 1], cut_in[lat : lat + 1])
            )
    cut_rows = jnp.concatenate(cuts * (PIECE // len(cuts)), axis=0)

    def gain_of(tile):
        j = lax.broadcasted_iota(jnp.int32, (PIECE, LANES), 1) + tile * LANES
        odd, within = j // wave_count, lax.rem(j, wave_count)
        wave = 2 * lax.rem(within, parity) + odd
        weight = jnp.where(wave == 0, 1.0, 2.0) / period
        return jnp.where(wave <= cut_rows, weight, 0.0).astype(F32)

    wave_tiles = spectra.shape[2] // LANES
    gains = jnp.concatenate([gain_of(tile) for tile in range(wave_tiles)], axis=1)

    def cross(i):
        return pltpu.make_async_remote_copy(
            src_ref=half_sum.at[pieces[i]],
            dst_ref=other_sum.at[pieces[i]],
            send_sem=cross_send.at[i],
            recv_sem=cross_recv.at[i],
            device_id=counterpart,
            device_id_type=MESH,
        )

    for i, piece in enumerate(pieces):
        here = arrived.at[:, piece]
        pltpu.make_async_copy(here, here, scatter_recv.at[i]).wait()
        total = arrived[0, piece]
        for sender in range(1, half_size):
            total += arrived[sender, piece]
        half_sum[piece] = total
        cross(i).start()
    pl.when(outer)(functools.partial(dense_start, first_part, second_part))
    for i, piece in enumerate(pieces):
        cross(i).wait_recv()
        scaled[piece] = (half_sum[piece] + other_sum[piece]) * gains
        to_half(
            lambda to: scaled.at[piece],
            gathered.at[place_in_half, piece],
            spread_send.at[i], spread_recv.at[i],
        )
    rest = first_part + second_part
    pl.when(outer)(functools.partial(dense_start, rest, levels - rest))

    def drain(offset):
        sent = slab.at[pl.ds(0, cols - 2 if offset == 1 else cols)]
        pltpu.make_async_copy(sent, sent, send_sem.at[offset]).wait()
        tag = tags_out.at[pl.ds(0, half_size - 1 if offset == 1 else half_size)]
        pltpu.make_async_copy(tag, tag, tag_send.at[offset]).wait()

    for offset in range(3):
        pl.when(valid(offset))(functools.partial(drain, offset))
    for i, piece in enumerate(pieces):
        others = arrived.at[pl.ds(0, half_size - 1), piece]
        pltpu.make_async_copy(others, others, scatter_send.at[i]).wait()
        cross(i).wait_send()

    def natural(spread):
        rows_of = [
            spread[row : row + lat_here]
            for level in range(levels)
            for row in (row_of(level, lat) for lat in range(0, lat_band, lat_here))
        ]
        return jnp.concatenate(rows_of, axis=0)[:, :longitudes].reshape(
            levels, lat_band, longitudes
        )

    for i, piece in enumerate(pieces):
        here = gathered.at[:, piece]
        pltpu.make_async_copy(here, here, spread_recv.at[i]).wait()
    spectrum = gathered[...].reshape(field_rows, 2 * wave_count)
    high, low = split(spectrum)
    both = dot(jnp.concatenate([high, low], axis=0), table_high[...], 1, 1)
    result = both[:field_rows] + both[field_rows:] + dot(high, table_low[...], 1, 1)
    filtered[...] = natural(result)

    pltpu.make_async_copy(passed, passed, pass_recv).wait()
    sums[:, :tile_count, :] += passed[...]
    for lat in range(lat_band):
        value = lat_rows(sums, lat)
        for level in range(levels):
            field[0, :, level * lat_band + lat, :] = value[level]
    rows_wide = jnp.concatenate([field[0, tile] for tile in range(long_tiles)], axis=1)
    remapped[...] = rows_wide[:, :longitudes].reshape(levels, lat_band, longitudes)

    pltpu.make_async_copy(passed, passed, pass_send).wait()
    for i, piece in enumerate(pieces):
        others = arrived.at[pl.ds(0, half_size - 1), piece]
        pltpu.make_async_copy(others, others, spread_send.at[i]).wait()


def cos_sin(positions):
    waves = np.concatenate([np.arange(0, KW, 2), np.arange(1, KW, 2)])
    phases = positions[:, None] * waves[None, :] % NLON
    angles = phases * (2 * np.pi / NLON)
    return np.cos(angles).astype(np.float32), np.sin(angles).astype(np.float32)


def local(mesh, source, weights, source_block, owner_device, target_tile, cutoff):
    bands, cols = mesh.shape["band"], mesh.shape["col"]
    levels = source.shape[0]
    block_count, block_width = weights.shape[:2]
    lat_here = cutoff.shape[0]
    lat_band = lat_here * cols
    half_size = cols // 2
    longitudes = NLON // cols
    cell_count = lat_band * longitudes
    tile_count = (cell_count + block_width - 1) // block_width
    regular = (tile_count + cols - 1) // cols
    capacity = regular + max(1, (block_count - cols * regular + 2 * cols - 1) // (2 * cols))
    capacity = round_up(capacity, 8)
    long_pad = round_up(longitudes, LANES)
    long_tiles = long_pad // LANES
    tiles = round_up(tile_count + long_tiles, LANES)
    sent_tiles = round_up(tile_count, 8)
    group_rows = levels * lat_band // half_size
    pieces = group_rows // PIECE
    chunks = block_count // CHUNK
    fine = np.stack(cos_sin(np.arange(STEP)))
    coarse = np.stack(cos_sin(STEP * np.arange(long_pad // STEP)), axis=1)
    start = np.stack(cos_sin(longitudes * np.arange(cols)), axis=1)

    slab_rows = levels * capacity
    smem = pl.BlockSpec(memory_space=pltpu.SMEM)
    vmem = pl.BlockSpec(memory_space=pltpu.VMEM)
    anywhere = pl.BlockSpec(memory_space=pl.ANY)
    shape = jax.ShapeDtypeStruct((levels, lat_band, longitudes), F32)
    dma = pltpu.SemaphoreType.DMA
    return pl.pallas_call(
        functools.partial(
            remap_kernel, bands, cols, levels, capacity, KW, NLON, longitudes, sent_tiles
        ),
        out_shape=(shape, shape),
        in_specs=[smem] * 2 + [vmem] * 5 + [anywhere] * 2,
        out_specs=(vmem, vmem),
        scratch_shapes=[
            pltpu.VMEM(weights.shape, BF16),
            pltpu.VMEM(source.shape, BF16),
            pltpu.VMEM((source.shape[1] // LANES, 16, LANES), BF16),
            pltpu.VMEM((source.shape[1] // LANES, 16, LANES), BF16),
            pltpu.VMEM((block_count, 8, LANES), F32),
            pltpu.VMEM((levels, tiles, LANES), F32),
            pltpu.VMEM((long_pad, 2 * KW), BF16),
            pltpu.VMEM((long_pad, 2 * KW), BF16),
            pltpu.VMEM((2, STEP, KW), F32),
            pltpu.VMEM((2, long_tiles, levels * lat_band, LANES), F32),
            pltpu.VMEM((3 * cols, slab_rows, LANES), F32),
            pltpu.VMEM((3 * half_size, slab_rows, LANES), F32),
            pltpu.VMEM((3 * half_size, slab_rows, LANES), F32),
            pltpu.VMEM((levels, tiles, LANES), F32),
            pltpu.VMEM((levels, sent_tiles, LANES), F32),
            pltpu.VMEM((3 * half_size, 2, LANES), F32),
            pltpu.VMEM((3 * half_size, 2, LANES), F32),
            pltpu.VMEM((lat_here, LANES), jnp.int32),
            pltpu.VMEM((lat_here, LANES), jnp.int32),
            pltpu.VMEM((half_size, group_rows, 2 * KW), F32),
            pltpu.VMEM((half_size, group_rows, 2 * KW), F32),
            pltpu.VMEM((group_rows, 2 * KW), F32),
            pltpu.VMEM((group_rows, 2 * KW), F32),
            pltpu.VMEM((group_rows, 2 * KW), F32),
            pltpu.VMEM((half_size, group_rows, 2 * KW), F32),
            dma((chunks,)),
            dma,
            dma((3,)),
            dma((3,)),
            dma,
            dma,
            dma((3,)),
            dma((3,)),
            dma((3,)),
            dma,
            dma,
            dma((pieces,)),
            dma((pieces,)),
            dma((pieces,)),
            dma((pieces,)),
            dma((pieces,)),
            dma((pieces,)),
        ],
        compiler_params=pltpu.CompilerParams(
            collective_id=0, has_side_effects=True, vmem_limit_bytes=56 << 20
        ),
    )(
        cutoff,
        source_block,
        owner_device.reshape(1, block_count),
        target_tile.reshape(1, block_count),
        fine,
        coarse,
        start,
        source,
        weights,
    )


def solution(mesh):
    in_specs = (
        P(None, ("band", "col")),
        P(("band", "col"), None, None),
        P(("band", "col")),
        P(("band", "col"), None),
        P(("band", "col")),
        P(("band", "col")),
    )
    out_specs = (P(None, "band", "col"), P(None, "band", "col"))
    return jax.shard_map(
        functools.partial(local, mesh),
        mesh=mesh,
        in_specs=in_specs,
        out_specs=out_specs,
        check_vma=False,
    )
```

```python
import functools

import jax
import jax.numpy as jnp
import numpy as np
from jax import lax
from jax.experimental import pallas as pl
from jax.experimental.pallas import tpu as pltpu
from jax.sharding import PartitionSpec as P

NLON = 7200
KW = 512
LANES = 128
STEP = 16
CHUNK = 32
PIECE = 8
DENSE = (0, 2, 3, 5, 6)
MESH = pl.DeviceIdType.MESH
F32 = jnp.float32
BF16 = jnp.bfloat16


def round_up(value, multiple):
    return (value + multiple - 1) // multiple * multiple


def split(value):
    high = value.astype(BF16)
    return high, (value - high.astype(F32)).astype(BF16)


def dot(left, right, left_dim=1, right_dim=0):
    return lax.dot_general(
        left, right, (((left_dim,), (right_dim,)), ((), ())), preferred_element_type=F32
    )


def remap_kernel(
    bands, cols, levels, capacity, wave_count, period, longitudes, tile_count,
    cutoff, source_block, owner_row, tile_row, fine, coarse, start, source, weights,
    remapped, filtered,
    weight_buf, source_even, source_odd, partial,
    sums, table_high, table_low, rotated, field, slab, recv, relay, relay_sums, passed,
    tags_out, tags_in, cut_out, cut_in,
    spectra, arrived, half_sum, other_sum, scaled, gathered,
    weight_sem, tag_send, tag_recv, cut_send, cut_recv,
    send_sem, recv_sem, relay_sem, pass_send, pass_recv,
    scatter_send, scatter_recv, cross_send, cross_recv, spread_send, spread_recv,
):
    band, col = lax.axis_index("band"), lax.axis_index("col")
    blocks = weights.shape[0]
    rows = levels * capacity
    half_size = cols // 2
    half, place_in_half = col // half_size, lax.rem(col, half_size)
    counterpart = (band, (1 - half) * half_size + place_in_half)

    def valid(offset):
        target = band + (offset - 1)
        return (target >= 0) & (target < bands)

    weight_copies = [
        pltpu.make_async_copy(
            weights.at[pl.ds(first, CHUNK)], weight_buf.at[pl.ds(first, CHUNK)], weight_sem.at[i]
        )
        for i, first in enumerate(range(0, blocks, CHUNK))
    ]
    for copy in weight_copies:
        copy.start()

    barrier = pltpu.get_barrier_semaphore()

    def greet(device):
        pl.semaphore_signal(barrier, inc=1, device_id=device, device_id_type=MESH)

    def greet_half(offset):
        def one(to, carry):
            def signal():
                greet((band + (offset - 1), half * half_size + to))

            if offset == 1:
                pl.when(to != place_in_half)(signal)
            else:
                signal()
            return carry

        lax.fori_loop(0, half_size, one, 0)

    for offset in (0, 2, 1):
        pl.when(valid(offset))(functools.partial(greet_half, offset))
    greet(counterpart)

    owners = owner_row[...]
    sublane = lax.broadcasted_iota(jnp.int32, (blocks, blocks), 0)
    lane = lax.broadcasted_iota(jnp.int32, (blocks, blocks), 1)
    owners_wide = jnp.broadcast_to(owners.astype(F32), (8, blocks))
    owner_column = jnp.transpose(owners_wide)[:, 0:1]
    earlier = (owner_column == owners.astype(F32)) & (sublane < lane)
    rank = jnp.sum(earlier.astype(jnp.int32), axis=0, keepdims=True)
    place = owners - (band - 1) * cols
    slot = place * capacity + rank
    slot_lane = lax.broadcasted_iota(jnp.int32, (LANES, blocks), 0)
    tile_at = jnp.where(slot_lane == rank, tile_row[...], 0).astype(F32).astype(BF16)
    place_ids = lax.broadcasted_iota(jnp.int32, (3 * cols, blocks), 0)
    chosen = (place_ids == place).astype(F32).astype(BF16)
    tags = dot(chosen, tile_at, 1, 1)
    for offset in range(3):
        for to in range(half_size):
            first = tags[offset * cols + to : offset * cols + to + 1]
            second = tags[offset * cols + half_size + to : offset * cols + half_size + to + 1]
            tags_out[offset * half_size + to, 0:1] = jnp.where(half == 0, first, second)
            tags_out[offset * half_size + to, 1:2] = jnp.where(half == 0, second, first)
    lat_here = cutoff.shape[0]
    for lat in range(lat_here):
        cut_out[lat : lat + 1] = jnp.full((1, LANES), cutoff[lat], jnp.int32)

    above = jnp.zeros((16 - levels, LANES), BF16)
    below = jnp.zeros((8, LANES), BF16)
    for index in range(source_even.shape[0]):
        value = source[:, index * LANES : (index + 1) * LANES]
        source_even[index] = jnp.concatenate([value, above], axis=0)
        source_odd[index] = jnp.concatenate([below, value, above[: 8 - levels]], axis=0)

    for i, copy in enumerate(weight_copies):
        copy.wait()
        for index in range(i * CHUNK, (i + 1) * CHUNK, 2):
            left = jnp.concatenate(
                [source_even[source_block[index]], source_odd[source_block[index + 1]]], axis=1
            )
            right = weight_buf[index : index + 2].reshape(2 * LANES, LANES)
            partial[index : index + 2] = dot(left, right).reshape(2, 8, LANES)

    inner_band = (band > 0) & (band < bands - 1)
    neighbours = jnp.where(inner_band, 2, 1) if bands > 1 else 0
    pl.semaphore_wait(barrier, half_size * (1 + neighbours))

    def send_to_half(source_of, target, sems_out, sems_in, offset):
        def one(step, carry):
            to = lax.rem(place_in_half + half_size // 2 + step, half_size)

            def start_remote():
                pltpu.make_async_remote_copy(
                    src_ref=source_of(to),
                    dst_ref=target,
                    send_sem=sems_out.at[offset],
                    recv_sem=sems_in.at[2 - offset],
                    device_id=(band + (offset - 1), half * half_size + to),
                    device_id_type=MESH,
                ).start()

            if offset == 1:
                pl.when(to != place_in_half)(start_remote)
            else:
                start_remote()
            return carry

        lax.fori_loop(0, half_size, one, 0)
        if offset == 1:
            pltpu.make_async_copy(source_of(place_in_half), target, sems_in.at[1]).start()

    def push_tags(offset):
        send_to_half(
            lambda to: tags_out.at[offset * half_size + to],
            tags_in.at[(2 - offset) * half_size + place_in_half],
            tag_send, tag_recv, offset,
        )

    def push(owner_half, into, sems, offset):
        send_to_half(
            lambda to: slab.at[offset * cols + owner_half * half_size + to],
            into.at[(2 - offset) * half_size + place_in_half],
            send_sem, sems, offset,
        )

    cut_copy = pltpu.make_async_remote_copy(
        src_ref=cut_out,
        dst_ref=cut_in,
        send_sem=cut_send,
        recv_sem=cut_recv,
        device_id=counterpart,
        device_id_type=MESH,
    )
    for offset in (0, 2, 1):
        pl.when(valid(offset))(functools.partial(push_tags, offset))
    cut_copy.start()

    data = jnp.concatenate([partial[:, level, :] for level in range(levels)], axis=1)
    stacked = jnp.concatenate(split(data), axis=0)

    def fill(offset):
        group = cols * capacity
        ids = lax.broadcasted_iota(jnp.int32, (group, blocks), 0) + offset * group
        placing = (ids == slot).astype(F32).astype(BF16)
        placed = dot(jnp.concatenate([placing, placing], axis=1), stacked)
        here = pl.ds(offset * cols, cols)
        for level in range(levels):
            piece = placed[:, level * LANES : (level + 1) * LANES]
            slab[here, level * capacity : (level + 1) * capacity, :] = piece.reshape(
                cols, capacity, LANES
            )

    def place_and_push(offset):
        fill(offset)
        push(1 - half, relay, relay_sem, offset)

    for offset in (0, 2, 1):
        pl.when(valid(offset))(functools.partial(place_and_push, offset))
    for offset in (0, 2, 1):
        pl.when(valid(offset))(functools.partial(push, half, recv, recv_sem, offset))

    begin = start[col]
    cos_start, sin_start = begin[0:1], begin[1:2]
    rotated[0] = fine[0] * cos_start - fine[1] * sin_start
    rotated[1] = fine[1] * cos_start + fine[0] * sin_start
    parity = wave_count // 2

    def table_step(step, carry):
        pair = coarse[step]
        cos_base, sin_base = pair[0:1], pair[1:2]
        cos_fine, sin_fine = rotated[0], rotated[1]
        at = pl.ds(pl.multiple_of(step * STEP, STEP), STEP)
        for first, value in (
            (0, cos_base * cos_fine - sin_base * sin_fine),
            (parity, sin_base * cos_fine + cos_base * sin_fine),
        ):
            high, low = split(value)
            for odd in range(2):
                here = slice(first + odd * wave_count, first + odd * wave_count + parity)
                there = slice(odd * parity, (odd + 1) * parity)
                table_high[at, here] = high[:, there]
                table_low[at, here] = low[:, there]
        return carry

    lax.fori_loop(0, coarse.shape[0], table_step, 0)

    tiles = sums.shape[1]
    sums[...] = jnp.zeros_like(sums)
    relay_sums[...] = jnp.zeros_like(relay_sums)

    def wait_tags(offset):
        here = tags_in.at[pl.ds(offset * half_size, half_size)]
        pltpu.make_async_copy(here, here, tag_recv.at[offset]).wait()

    for offset in (0, 2, 1):
        pl.when(valid(offset))(functools.partial(wait_tags, offset))

    def receive(ref, sems, into, kind, offset):
        here = pl.ds(offset * half_size, half_size)
        tag_rows = [
            tags_in[offset * half_size + sender, kind : kind + 1] for sender in range(half_size)
        ]
        tags = jnp.transpose(jnp.concatenate(tag_rows * (-(-8 // half_size)), axis=0))
        wide = lax.broadcasted_iota(jnp.int32, (capacity, tiles), 1).astype(F32)
        chooser = jnp.concatenate(
            [
                (tags[:capacity, sender : sender + 1] == wide).astype(F32)
                for sender in range(half_size)
            ],
            axis=0,
        )
        chooser = jnp.transpose(chooser).astype(BF16)
        pltpu.make_async_copy(ref.at[here], ref.at[here], sems.at[offset]).wait()
        incoming = jnp.concatenate(
            [
                ref[here, level * capacity : (level + 1) * capacity, :].reshape(
                    half_size * capacity, LANES
                )
                for level in range(levels)
            ],
            axis=1,
        )
        high, low = split(incoming)
        total = dot(chooser, high) + dot(chooser, low)
        for level in range(levels):
            into[level] += total[:, level * LANES : (level + 1) * LANES]

    def dense_start(first, count):
        here = (pl.ds(first, count), pl.ds(0, tile_count))
        pltpu.make_async_remote_copy(
            src_ref=relay_sums.at[here],
            dst_ref=passed.at[pl.ds(first, count)],
            send_sem=pass_send,
            recv_sem=pass_recv,
            device_id=counterpart,
            device_id_type=MESH,
        ).start()

    ends = [levels * share // DENSE[-1] for share in DENSE]

    def dense_part(index):
        if ends[index + 1] > ends[index]:
            dense_start(ends[index], ends[index + 1] - ends[index])

    for offset in (0, 2, 1):
        pl.when(valid(offset))(functools.partial(receive, relay, relay_sem, relay_sums, 1, offset))
    dense_part(0)
    for offset in (0, 2, 1):
        pl.when(valid(offset))(functools.partial(receive, recv, recv_sem, sums, 0, offset))

    long_tiles, field_rows = field.shape[1:3]
    lat_band = field_rows // levels
    group_rows = field_rows // half_size
    shape3 = (levels, long_tiles, LANES)
    lane3 = lax.broadcasted_iota(jnp.int32, shape3, 2)
    inside = lax.broadcasted_iota(jnp.int32, shape3, 1) * LANES + lane3 < longitudes

    def row_of(level, lat):
        owner, within = divmod(lat, lat_here)
        lat_half, owner_place = divmod(owner, half_size)
        return owner_place * group_rows + (level * 2 + lat_half) * lat_here + within

    def lat_rows(ref, lat):
        first, shift = divmod(lat * longitudes, LANES)
        value = ref[:, first : first + long_tiles, :]
        if shift:
            after = ref[:, first + 1 : first + 1 + long_tiles, :]
            value = jnp.where(
                lane3 < LANES - shift,
                pltpu.roll(value, LANES - shift, 2),
                pltpu.roll(after, LANES - shift, 2),
            )
        return jnp.where(inside, value, 0.0)

    for lat in range(lat_band):
        own, relayed = lat_rows(sums, lat), lat_rows(relay_sums, lat)
        both, apart = own + relayed, own - relayed
        for level in range(levels):
            field[0, :, row_of(level, lat), :] = both[level]
            field[1, :, row_of(level, lat), :] = apart[level]

    for odd in range(2):
        rows_wide = jnp.concatenate([field[odd, tile] for tile in range(long_tiles)], axis=1)
        high, low = split(rows_wide)
        waves = slice(odd * wave_count, (odd + 1) * wave_count)
        both = dot(jnp.concatenate([high, low], axis=0), table_high[:, waves])
        spectrum = both[:field_rows] + both[field_rows:] + dot(high, table_low[:, waves])
        spectra[:, :, waves] = spectrum.reshape(half_size, group_rows, wave_count)

    pieces = [pl.ds(first, PIECE) for first in range(0, group_rows, PIECE)]

    def to_half(source_of, target, sem_out, sem_in):
        def one(step, carry):
            to = lax.rem(place_in_half + half_size // 2 + step, half_size)

            def start_remote():
                pltpu.make_async_remote_copy(
                    src_ref=source_of(to),
                    dst_ref=target,
                    send_sem=sem_out,
                    recv_sem=sem_in,
                    device_id=(band, half * half_size + to),
                    device_id_type=MESH,
                ).start()

            pl.when(to != place_in_half)(start_remote)
            return carry

        lax.fori_loop(0, half_size, one, 0)
        pltpu.make_async_copy(source_of(place_in_half), target, sem_in).start()

    for i, piece in enumerate(pieces):
        to_half(
            lambda to: spectra.at[to, piece],
            arrived.at[place_in_half, piece],
            scatter_send.at[i], scatter_recv.at[i],
        )
    dense_part(1)

    cut_copy.wait()
    cuts = []
    for lat_half in range(2):
        for lat in range(lat_here):
            cuts.append(
                jnp.where(half == lat_half, cut_out[lat : lat + 1], cut_in[lat : lat + 1])
            )
    cut_rows = jnp.concatenate(cuts * (PIECE // len(cuts)), axis=0)

    def gain_of(tile):
        j = lax.broadcasted_iota(jnp.int32, (PIECE, LANES), 1) + tile * LANES
        odd, within = j // wave_count, lax.rem(j, wave_count)
        wave = 2 * lax.rem(within, parity) + odd
        weight = jnp.where(wave == 0, 1.0, 2.0) / period
        return jnp.where(wave <= cut_rows, weight, 0.0).astype(F32)

    wave_tiles = spectra.shape[2] // LANES
    gains = jnp.concatenate([gain_of(tile) for tile in range(wave_tiles)], axis=1)

    def cross(i):
        return pltpu.make_async_remote_copy(
            src_ref=half_sum.at[pieces[i]],
            dst_ref=other_sum.at[pieces[i]],
            send_sem=cross_send.at[i],
            recv_sem=cross_recv.at[i],
            device_id=counterpart,
            device_id_type=MESH,
        )

    for i, piece in enumerate(pieces):
        here = arrived.at[:, piece]
        pltpu.make_async_copy(here, here, scatter_recv.at[i]).wait()
        total = arrived[0, piece]
        for sender in range(1, half_size):
            total += arrived[sender, piece]
        half_sum[piece] = total
        cross(i).start()
    dense_part(2)
    for i, piece in enumerate(pieces):
        cross(i).wait_recv()
        scaled[piece] = (half_sum[piece] + other_sum[piece]) * gains
        to_half(
            lambda to: scaled.at[piece],
            gathered.at[place_in_half, piece],
            spread_send.at[i], spread_recv.at[i],
        )
    dense_part(3)

    def drain(offset):
        sent = slab.at[pl.ds(0, cols - 2 if offset == 1 else cols)]
        pltpu.make_async_copy(sent, sent, send_sem.at[offset]).wait()
        tag = tags_out.at[pl.ds(0, half_size - 1 if offset == 1 else half_size)]
        pltpu.make_async_copy(tag, tag, tag_send.at[offset]).wait()

    for offset in range(3):
        pl.when(valid(offset))(functools.partial(drain, offset))
    for i, piece in enumerate(pieces):
        others = arrived.at[pl.ds(0, half_size - 1), piece]
        pltpu.make_async_copy(others, others, scatter_send.at[i]).wait()
        cross(i).wait_send()

    def natural(spread):
        rows_of = [
            spread[row : row + lat_here]
            for level in range(levels)
            for row in (row_of(level, lat) for lat in range(0, lat_band, lat_here))
        ]
        return jnp.concatenate(rows_of, axis=0)[:, :longitudes].reshape(
            levels, lat_band, longitudes
        )

    for i, piece in enumerate(pieces):
        here = gathered.at[:, piece]
        pltpu.make_async_copy(here, here, spread_recv.at[i]).wait()
    spectrum = gathered[...].reshape(field_rows, 2 * wave_count)
    high, low = split(spectrum)
    both = dot(jnp.concatenate([high, low], axis=0), table_high[...], 1, 1)
    result = both[:field_rows] + both[field_rows:] + dot(high, table_low[...], 1, 1)
    filtered[...] = natural(result)

    pltpu.make_async_copy(passed, passed, pass_recv).wait()
    sums[:, :tile_count, :] += passed[...]
    for lat in range(lat_band):
        value = lat_rows(sums, lat)
        for level in range(levels):
            field[0, :, level * lat_band + lat, :] = value[level]
    rows_wide = jnp.concatenate([field[0, tile] for tile in range(long_tiles)], axis=1)
    remapped[...] = rows_wide[:, :longitudes].reshape(levels, lat_band, longitudes)

    pltpu.make_async_copy(passed, passed, pass_send).wait()
    for i, piece in enumerate(pieces):
        others = arrived.at[pl.ds(0, half_size - 1), piece]
        pltpu.make_async_copy(others, others, spread_send.at[i]).wait()


def cos_sin(positions):
    waves = np.concatenate([np.arange(0, KW, 2), np.arange(1, KW, 2)])
    phases = positions[:, None] * waves[None, :] % NLON
    angles = phases * (2 * np.pi / NLON)
    return np.cos(angles).astype(np.float32), np.sin(angles).astype(np.float32)


def local(mesh, source, weights, source_block, owner_device, target_tile, cutoff):
    bands, cols = mesh.shape["band"], mesh.shape["col"]
    levels = source.shape[0]
    block_count, block_width = weights.shape[:2]
    lat_here = cutoff.shape[0]
    lat_band = lat_here * cols
    half_size = cols // 2
    longitudes = NLON // cols
    cell_count = lat_band * longitudes
    tile_count = (cell_count + block_width - 1) // block_width
    regular = (tile_count + cols - 1) // cols
    capacity = regular + max(1, (block_count - cols * regular + 2 * cols - 1) // (2 * cols))
    capacity = round_up(capacity, 8)
    long_pad = round_up(longitudes, LANES)
    long_tiles = long_pad // LANES
    tiles = round_up(tile_count + long_tiles, LANES)
    sent_tiles = round_up(tile_count, 8)
    group_rows = levels * lat_band // half_size
    pieces = group_rows // PIECE
    chunks = block_count // CHUNK
    fine = np.stack(cos_sin(np.arange(STEP)))
    coarse = np.stack(cos_sin(STEP * np.arange(long_pad // STEP)), axis=1)
    start = np.stack(cos_sin(longitudes * np.arange(cols)), axis=1)

    slab_rows = levels * capacity
    smem = pl.BlockSpec(memory_space=pltpu.SMEM)
    vmem = pl.BlockSpec(memory_space=pltpu.VMEM)
    anywhere = pl.BlockSpec(memory_space=pl.ANY)
    shape = jax.ShapeDtypeStruct((levels, lat_band, longitudes), F32)
    dma = pltpu.SemaphoreType.DMA
    return pl.pallas_call(
        functools.partial(
            remap_kernel, bands, cols, levels, capacity, KW, NLON, longitudes, sent_tiles
        ),
        out_shape=(shape, shape),
        in_specs=[smem] * 2 + [vmem] * 6 + [anywhere],
        out_specs=(vmem, vmem),
        scratch_shapes=[
            pltpu.VMEM(weights.shape, BF16),
            pltpu.VMEM((source.shape[1] // LANES, 16, LANES), BF16),
            pltpu.VMEM((source.shape[1] // LANES, 16, LANES), BF16),
            pltpu.VMEM((block_count, 8, LANES), F32),
            pltpu.VMEM((levels, tiles, LANES), F32),
            pltpu.VMEM((long_pad, 2 * KW), BF16),
            pltpu.VMEM((long_pad, 2 * KW), BF16),
            pltpu.VMEM((2, STEP, KW), F32),
            pltpu.VMEM((2, long_tiles, levels * lat_band, LANES), F32),
            pltpu.VMEM((3 * cols, slab_rows, LANES), F32),
            pltpu.VMEM((3 * half_size, slab_rows, LANES), F32),
            pltpu.VMEM((3 * half_size, slab_rows, LANES), F32),
            pltpu.VMEM((levels, tiles, LANES), F32),
            pltpu.VMEM((levels, sent_tiles, LANES), F32),
            pltpu.VMEM((3 * half_size, 2, LANES), F32),
            pltpu.VMEM((3 * half_size, 2, LANES), F32),
            pltpu.VMEM((lat_here, LANES), jnp.int32),
            pltpu.VMEM((lat_here, LANES), jnp.int32),
            pltpu.VMEM((half_size, group_rows, 2 * KW), F32),
            pltpu.VMEM((half_size, group_rows, 2 * KW), F32),
            pltpu.VMEM((group_rows, 2 * KW), F32),
            pltpu.VMEM((group_rows, 2 * KW), F32),
            pltpu.VMEM((group_rows, 2 * KW), F32),
            pltpu.VMEM((half_size, group_rows, 2 * KW), F32),
            dma((chunks,)),
            dma((3,)),
            dma((3,)),
            dma,
            dma,
            dma((3,)),
            dma((3,)),
            dma((3,)),
            dma,
            dma,
            dma((pieces,)),
            dma((pieces,)),
            dma((pieces,)),
            dma((pieces,)),
            dma((pieces,)),
            dma((pieces,)),
        ],
        compiler_params=pltpu.CompilerParams(
            collective_id=0, has_side_effects=True, vmem_limit_bytes=56 << 20
        ),
    )(
        cutoff,
        source_block,
        owner_device.reshape(1, block_count),
        target_tile.reshape(1, block_count),
        fine,
        coarse,
        start,
        source,
        weights,
    )


def solution(mesh):
    in_specs = (
        P(None, ("band", "col")),
        P(("band", "col"), None, None),
        P(("band", "col")),
        P(("band", "col"), None),
        P(("band", "col")),
        P(("band", "col")),
    )
    out_specs = (P(None, "band", "col"), P(None, "band", "col"))
    return jax.shard_map(
        functools.partial(local, mesh),
        mesh=mesh,
        in_specs=in_specs,
        out_specs=out_specs,
        check_vma=False,
    )
```

```python
import functools

import jax
import jax.numpy as jnp
import numpy as np
from jax import lax
from jax.experimental import pallas as pl
from jax.experimental.pallas import tpu as pltpu
from jax.sharding import PartitionSpec as P

NLON = 7200
KW = 512
LANES = 128
STEP = 16
CHUNK = 32
PIECE = 256
TOGETHER = 4
DENSE = (0, 4, 4, 4, 6)
MESH = pl.DeviceIdType.MESH
F32 = jnp.float32
BF16 = jnp.bfloat16


def round_up(value, multiple):
    return (value + multiple - 1) // multiple * multiple


def split(value):
    high = value.astype(BF16)
    return high, (value - high.astype(F32)).astype(BF16)


def dot(left, right, left_dim=1, right_dim=0):
    return lax.dot_general(
        left, right, (((left_dim,), (right_dim,)), ((), ())), preferred_element_type=F32
    )


def remap_kernel(
    bands, cols, width, levels, capacity, wave_count, period, longitudes, tile_count,
    cutoff, source_block, owner_row, tile_row, fine, coarse, start, turn, source, weights,
    remapped, filtered,
    weight_buf, source_even, source_odd, partial,
    sums, table_high, table_low, rotated, field, slab, recv, relay, relay_sums, passed,
    tags_out, tags_in, cut_out, cut_in,
    spectra, arrived, half_sum, other_sum, scaled, gathered,
    weight_sem, tag_send, tag_recv, cut_send, cut_recv,
    send_sem, recv_sem, relay_sem, pass_send, pass_recv,
    scatter_send, scatter_recv, cross_send, cross_recv, spread_send, spread_recv,
):
    band, col = lax.axis_index("band"), lax.axis_index("col")
    blocks = weights.shape[0]
    rows = levels * capacity
    half_size = cols // 2
    half, place_in_half = col // half_size, lax.rem(col, half_size)
    layers = half_size // width
    layer = place_in_half // width

    def mirror(where):
        return (layers - 1 - where // width) * width + where % width

    def group_of(where):
        return jnp.where(half == 0, where, mirror(where))

    counterpart = (band, (1 - half) * half_size + mirror(place_in_half))

    def valid(offset):
        target = band + (offset - 1)
        return (target >= 0) & (target < bands)

    weight_copies = [
        pltpu.make_async_copy(
            weights.at[pl.ds(first, CHUNK)], weight_buf.at[pl.ds(first, CHUNK)], weight_sem.at[i]
        )
        for i, first in enumerate(range(0, blocks, CHUNK))
    ]
    for copy in weight_copies:
        copy.start()

    barrier = pltpu.get_barrier_semaphore()

    def greet(device):
        pl.semaphore_signal(barrier, inc=1, device_id=device, device_id_type=MESH)

    def greet_half(offset):
        def one(to, carry):
            def signal():
                greet((band + (offset - 1), half * half_size + to))

            if offset == 1:
                pl.when(to != place_in_half)(signal)
            else:
                signal()
            return carry

        lax.fori_loop(0, half_size, one, 0)

    for offset in (0, 2, 1):
        pl.when(valid(offset))(functools.partial(greet_half, offset))
    greet(counterpart)

    owners = owner_row[...]
    sublane = lax.broadcasted_iota(jnp.int32, (blocks, blocks), 0)
    lane = lax.broadcasted_iota(jnp.int32, (blocks, blocks), 1)
    owners_wide = jnp.broadcast_to(owners.astype(F32), (8, blocks))
    owner_column = jnp.transpose(owners_wide)[:, 0:1]
    earlier = (owner_column == owners.astype(F32)) & (sublane < lane)
    rank = jnp.sum(earlier.astype(jnp.int32), axis=0, keepdims=True)
    place = owners - (band - 1) * cols
    slot = place * capacity + rank
    slot_lane = lax.broadcasted_iota(jnp.int32, (LANES, blocks), 0)
    tile_at = jnp.where(slot_lane == rank, tile_row[...], 0).astype(F32).astype(BF16)
    place_ids = lax.broadcasted_iota(jnp.int32, (3 * cols, blocks), 0)
    chosen = (place_ids == place).astype(F32).astype(BF16)
    tags = dot(chosen, tile_at, 1, 1)
    for offset in range(3):
        for to in range(half_size):
            here = [
                tags[row : row + 1]
                for row in (
                    offset * cols + lat_half * half_size + where
                    for where in (to, mirror(to))
                    for lat_half in range(2)
                )
            ]
            tags_out[offset * half_size + to, 0:1] = jnp.where(half == 0, here[0], here[1])
            tags_out[offset * half_size + to, 1:2] = jnp.where(half == 0, here[3], here[2])
    lat_here = cutoff.shape[0]
    for lat in range(lat_here):
        cut_out[lat : lat + 1] = jnp.full((1, LANES), cutoff[lat], jnp.int32)

    above = jnp.zeros((16 - levels, LANES), BF16)
    below = jnp.zeros((8, LANES), BF16)
    for index in range(source_even.shape[0]):
        value = source[:, index * LANES : (index + 1) * LANES]
        source_even[index] = jnp.concatenate([value, above], axis=0)
        source_odd[index] = jnp.concatenate([below, value, above[: 8 - levels]], axis=0)

    for i, copy in enumerate(weight_copies):
        copy.wait()
        for index in range(i * CHUNK, (i + 1) * CHUNK, 2):
            left = jnp.concatenate(
                [source_even[source_block[index]], source_odd[source_block[index + 1]]], axis=1
            )
            right = weight_buf[index : index + 2].reshape(2 * LANES, LANES)
            partial[index : index + 2] = dot(left, right).reshape(2, 8, LANES)

    data = jnp.concatenate([partial[:, level, :] for level in range(levels)], axis=1)
    stacked = jnp.concatenate(split(data), axis=0)

    def fill(offset):
        group = cols * capacity
        ids = lax.broadcasted_iota(jnp.int32, (group, blocks), 0) + offset * group
        placing = (ids == slot).astype(F32).astype(BF16)
        placed = dot(jnp.concatenate([placing, placing], axis=1), stacked)
        here = pl.ds(offset * cols, cols)
        for level in range(levels):
            piece = placed[:, level * LANES : (level + 1) * LANES]
            slab[here, level * capacity : (level + 1) * capacity, :] = piece.reshape(
                cols, capacity, LANES
            )

    pl.when(valid(0))(functools.partial(fill, 0))
    pl.when(band == 0)(functools.partial(fill, 2))

    inner_band = (band > 0) & (band < bands - 1)
    neighbours = jnp.where(inner_band, 2, 1) if bands > 1 else 0
    pl.semaphore_wait(barrier, half_size * (1 + neighbours))

    def send_to_half(source_of, target, sems_out, sems_in, offset):
        def one(step, carry):
            to = lax.rem(place_in_half + half_size // 2 + step, half_size)

            def start_remote():
                pltpu.make_async_remote_copy(
                    src_ref=source_of(to),
                    dst_ref=target,
                    send_sem=sems_out.at[offset],
                    recv_sem=sems_in.at[2 - offset],
                    device_id=(band + (offset - 1), half * half_size + to),
                    device_id_type=MESH,
                ).start()

            if offset == 1:
                pl.when(to != place_in_half)(start_remote)
            else:
                start_remote()
            return carry

        lax.fori_loop(0, half_size, one, 0)
        if offset == 1:
            pltpu.make_async_copy(source_of(place_in_half), target, sems_in.at[1]).start()

    def push_tags(offset):
        send_to_half(
            lambda to: tags_out.at[offset * half_size + to],
            tags_in.at[(2 - offset) * half_size + place_in_half],
            tag_send, tag_recv, offset,
        )

    def push(owner_half, owner_of, into, sems, offset):
        send_to_half(
            lambda to: slab.at[offset * cols + owner_half * half_size + owner_of(to)],
            into.at[(2 - offset) * half_size + place_in_half],
            send_sem, sems, offset,
        )

    cut_copy = pltpu.make_async_remote_copy(
        src_ref=cut_out,
        dst_ref=cut_in,
        send_sem=cut_send,
        recv_sem=cut_recv,
        device_id=counterpart,
        device_id_type=MESH,
    )
    for offset in (0, 2, 1):
        pl.when(valid(offset))(functools.partial(push_tags, offset))
    cut_copy.start()

    def place_and_push(offset):
        if offset == 1:
            fill(offset)
        elif offset == 2:
            pl.when(band > 0)(functools.partial(fill, offset))
        push(1 - half, mirror, relay, relay_sem, offset)

    for offset in (0, 2, 1):
        pl.when(valid(offset))(functools.partial(place_and_push, offset))
    for offset in (0, 2, 1):
        pl.when(valid(offset))(functools.partial(push, half, lambda to: to, recv, recv_sem, offset))

    begin = start[col]
    cos_start, sin_start = begin[0:1], begin[1:2]
    rotated[0] = fine[0] * cos_start - fine[1] * sin_start
    rotated[1] = fine[1] * cos_start + fine[0] * sin_start

    def table_step(step, carry):
        pair = coarse[step]
        cos_base, sin_base = pair[0:1], pair[1:2]
        cos_fine, sin_fine = rotated[0], rotated[1]
        at = pl.ds(pl.multiple_of(step * STEP, STEP), STEP)
        for first, value in (
            (0, cos_base * cos_fine - sin_base * sin_fine),
            (wave_count, sin_base * cos_fine + cos_base * sin_fine),
        ):
            high, low = split(value)
            table_high[at, first : first + wave_count] = high
            table_low[at, first : first + wave_count] = low
        return carry

    lax.fori_loop(0, coarse.shape[0], table_step, 0)

    tiles = sums.shape[1]
    sums[...] = jnp.zeros_like(sums)
    relay_sums[...] = jnp.zeros_like(relay_sums)

    def wait_tags(offset):
        here = tags_in.at[pl.ds(offset * half_size, half_size)]
        pltpu.make_async_copy(here, here, tag_recv.at[offset]).wait()

    for offset in (0, 2, 1):
        pl.when(valid(offset))(functools.partial(wait_tags, offset))

    def receive(ref, sems, into, kind, offset):
        here = pl.ds(offset * half_size, half_size)
        tag_rows = [
            tags_in[offset * half_size + sender, kind : kind + 1] for sender in range(half_size)
        ]
        tags = jnp.transpose(jnp.concatenate(tag_rows * (-(-8 // half_size)), axis=0))
        wide = lax.broadcasted_iota(jnp.int32, (capacity, tiles), 1).astype(F32)
        chooser = jnp.concatenate(
            [
                (tags[:capacity, sender : sender + 1] == wide).astype(F32)
                for sender in range(half_size)
            ],
            axis=0,
        )
        chooser = jnp.transpose(chooser).astype(BF16)
        pltpu.make_async_copy(ref.at[here], ref.at[here], sems.at[offset]).wait()
        incoming = jnp.concatenate(
            [
                ref[here, level * capacity : (level + 1) * capacity, :].reshape(
                    half_size * capacity, LANES
                )
                for level in range(levels)
            ],
            axis=1,
        )
        high, low = split(incoming)
        total = dot(chooser, high) + dot(chooser, low)
        for level in range(levels):
            into[level] += total[:, level * LANES : (level + 1) * LANES]

    def dense_start(first, count):
        here = (pl.ds(first, count), pl.ds(0, tile_count))
        pltpu.make_async_remote_copy(
            src_ref=relay_sums.at[here],
            dst_ref=passed.at[pl.ds(first, count)],
            send_sem=pass_send,
            recv_sem=pass_recv,
            device_id=counterpart,
            device_id_type=MESH,
        ).start()

    inner = jnp.where(half == 0, layer >= layers // 2, layer < layers - layers // 2)
    outer = jnp.logical_not(inner)
    ends = [levels * share // DENSE[-1] for share in DENSE]

    def dense_part(index):
        if ends[index + 1] > ends[index]:
            pl.when(outer)(
                functools.partial(dense_start, ends[index], ends[index + 1] - ends[index])
            )

    for offset in (0, 2, 1):
        pl.when(valid(offset))(functools.partial(receive, relay, relay_sem, relay_sums, 1, offset))
    pl.when(inner)(functools.partial(dense_start, 0, levels))
    dense_part(0)

    long_tiles, field_rows = field.shape[1:3]
    lat_band = field_rows // levels
    group_rows = field_rows // half_size
    shape3 = (levels, long_tiles, LANES)
    lane3 = lax.broadcasted_iota(jnp.int32, shape3, 2)
    inside = lax.broadcasted_iota(jnp.int32, shape3, 1) * LANES + lane3 < longitudes

    def row_of(level, lat):
        owner, within = divmod(lat, lat_here)
        lat_half, owner_place = divmod(owner, half_size)
        group = mirror(owner_place) if lat_half else owner_place
        return group * group_rows + (level * 2 + lat_half) * lat_here + within

    def lat_rows(ref, lat):
        first, shift = divmod(lat * longitudes, LANES)
        value = ref[:, first : first + long_tiles, :]
        if shift:
            after = ref[:, first + 1 : first + 1 + long_tiles, :]
            value = jnp.where(
                lane3 < LANES - shift,
                pltpu.roll(value, LANES - shift, 2),
                pltpu.roll(after, LANES - shift, 2),
            )
        return jnp.where(inside, value, 0.0)

    def rows_of_field(ref, index):
        for lat in range(lat_band):
            value = lat_rows(ref, lat)
            for level in range(levels):
                field[index, :, row_of(level, lat), :] = value[level]
        rows_wide = jnp.concatenate([field[index, tile] for tile in range(long_tiles)], axis=1)
        high, low = split(rows_wide)
        return jnp.concatenate([high, low], axis=0), high

    def transformed(parts, waves):
        both = dot(parts[0], table_high[:, waves])
        return both[:field_rows] + both[field_rows:] + dot(parts[1], table_low[:, waves])

    relayed = transformed(rows_of_field(relay_sums, 1), slice(None))
    angle = turn[col]
    cos_part, sin_part = relayed[:, :wave_count], relayed[:, wave_count:]
    grouped = (half_size, group_rows, wave_count)
    spectra[:, :, :wave_count] = (cos_part * angle[0:1] - sin_part * angle[1:2]).reshape(grouped)
    spectra[:, :, wave_count:] = (sin_part * angle[0:1] + cos_part * angle[1:2]).reshape(grouped)

    for offset in (0, 2, 1):
        pl.when(valid(offset))(functools.partial(receive, recv, recv_sem, sums, 0, offset))

    waves = 2 * wave_count
    pieces = [slice(first, first + PIECE) for first in range(0, waves, PIECE)]

    def to_half(source_of, target, sem_out, sem_in):
        def one(step, carry):
            to = lax.rem(place_in_half + half_size // 2 + step, half_size)

            def start_remote():
                pltpu.make_async_remote_copy(
                    src_ref=source_of(to),
                    dst_ref=target,
                    send_sem=sem_out,
                    recv_sem=sem_in,
                    device_id=(band, half * half_size + to),
                    device_id_type=MESH,
                ).start()

            pl.when(to != place_in_half)(start_remote)
            return carry

        lax.fori_loop(0, half_size, one, 0)
        pltpu.make_async_copy(source_of(place_in_half), target, sem_in).start()

    parts = rows_of_field(sums, 0)
    for i, piece in enumerate(pieces):
        if i % TOGETHER == 0:
            wide = slice(piece.start, piece.start + TOGETHER * PIECE)
            spectra[:, :, wide] += transformed(parts, wide).reshape(
                half_size, group_rows, TOGETHER * PIECE
            )
        to_half(
            lambda to: spectra.at[group_of(to), :, piece],
            arrived.at[place_in_half, :, piece],
            scatter_send.at[i], scatter_recv.at[i],
        )
    dense_part(1)

    cut_copy.wait()
    cuts = []
    for lat_half in range(2):
        for lat in range(lat_here):
            cuts.append(
                jnp.where(half == lat_half, cut_out[lat : lat + 1], cut_in[lat : lat + 1])
            )
    cut_rows = jnp.concatenate(cuts * (group_rows // len(cuts)), axis=0)

    def gain_of(tile):
        j = lax.broadcasted_iota(jnp.int32, (group_rows, LANES), 1) + tile * LANES
        wave = jnp.where(j >= wave_count, j - wave_count, j)
        weight = jnp.where(wave == 0, 1.0, 2.0) / period
        return jnp.where(wave <= cut_rows, weight, 0.0).astype(F32)

    gains = jnp.concatenate([gain_of(tile) for tile in range(waves // LANES)], axis=1)

    def cross(i):
        return pltpu.make_async_remote_copy(
            src_ref=half_sum.at[:, pieces[i]],
            dst_ref=other_sum.at[:, pieces[i]],
            send_sem=cross_send.at[i],
            recv_sem=cross_recv.at[i],
            device_id=counterpart,
            device_id_type=MESH,
        )

    for i, piece in enumerate(pieces):
        here = arrived.at[:, :, piece]
        pltpu.make_async_copy(here, here, scatter_recv.at[i]).wait()
        total = arrived[0, :, piece]
        for sender in range(1, half_size):
            total += arrived[sender, :, piece]
        half_sum[:, piece] = total
        cross(i).start()
    dense_part(2)
    for i, piece in enumerate(pieces):
        cross(i).wait_recv()
        scaled[:, piece] = (half_sum[:, piece] + other_sum[:, piece]) * gains[:, piece]
        to_half(
            lambda to: scaled.at[:, piece],
            gathered.at[group_of(place_in_half), :, piece],
            spread_send.at[i], spread_recv.at[i],
        )
    dense_part(3)

    def drain(offset):
        sent = slab.at[pl.ds(0, cols - 2 if offset == 1 else cols)]
        pltpu.make_async_copy(sent, sent, send_sem.at[offset]).wait()
        tag = tags_out.at[pl.ds(0, half_size - 1 if offset == 1 else half_size)]
        pltpu.make_async_copy(tag, tag, tag_send.at[offset]).wait()

    for offset in range(3):
        pl.when(valid(offset))(functools.partial(drain, offset))
    for i, piece in enumerate(pieces):
        others = arrived.at[pl.ds(0, half_size - 1), :, piece]
        pltpu.make_async_copy(others, others, scatter_send.at[i]).wait()
        cross(i).wait_send()

    def natural(spread):
        rows_of = [
            spread[row : row + lat_here]
            for level in range(levels)
            for row in (row_of(level, lat) for lat in range(0, lat_band, lat_here))
        ]
        return jnp.concatenate(rows_of, axis=0)[:, :longitudes].reshape(
            levels, lat_band, longitudes
        )

    result = None
    for i, piece in enumerate(pieces):
        here = gathered.at[:, :, piece]
        pltpu.make_async_copy(here, here, spread_recv.at[i]).wait()
        high, low = split(gathered[:, :, piece].reshape(field_rows, PIECE))
        both = dot(jnp.concatenate([high, low], axis=0), table_high[:, piece], 1, 1)
        added = both[:field_rows] + both[field_rows:] + dot(high, table_low[:, piece], 1, 1)
        result = added if result is None else result + added
    filtered[...] = natural(result)

    pltpu.make_async_copy(passed, passed, pass_recv).wait()
    sums[:, :tile_count, :] += passed[...]
    for lat in range(lat_band):
        value = lat_rows(sums, lat)
        for level in range(levels):
            field[0, :, level * lat_band + lat, :] = value[level]
    rows_wide = jnp.concatenate([field[0, tile] for tile in range(long_tiles)], axis=1)
    remapped[...] = rows_wide[:, :longitudes].reshape(levels, lat_band, longitudes)

    pltpu.make_async_copy(passed, passed, pass_send).wait()
    for i, piece in enumerate(pieces):
        others = arrived.at[pl.ds(0, half_size - 1), :, piece]
        pltpu.make_async_copy(others, others, spread_send.at[i]).wait()


def deliver(first, second, first_out, second_out, sem):
    copies = [
        pltpu.make_async_copy(first, first_out, sem.at[0]),
        pltpu.make_async_copy(second, second_out, sem.at[1]),
    ]
    for copy in copies:
        copy.start()
    for copy in copies:
        copy.wait()


def cos_sin(positions):
    phases = positions[:, None] * np.arange(KW)[None, :] % NLON
    angles = phases * (2 * np.pi / NLON)
    return np.cos(angles).astype(np.float32), np.sin(angles).astype(np.float32)


def width_of(mesh):
    cols = mesh.shape["col"]
    places = [getattr(device, "coords", None) for device in mesh.devices[0]]
    if None in places:
        return 1
    width = sum(place[2] == places[0][2] for place in places)
    return width if cols % (2 * width) == 0 else 1


def local(mesh, source, weights, source_block, owner_device, target_tile, cutoff):
    bands, cols = mesh.shape["band"], mesh.shape["col"]
    levels = source.shape[0]
    block_count, block_width = weights.shape[:2]
    lat_here = cutoff.shape[0]
    lat_band = lat_here * cols
    half_size = cols // 2
    longitudes = NLON // cols
    cell_count = lat_band * longitudes
    tile_count = (cell_count + block_width - 1) // block_width
    regular = (tile_count + cols - 1) // cols
    capacity = regular + max(1, (block_count - cols * regular + 2 * cols - 1) // (2 * cols))
    capacity = round_up(capacity, 8)
    long_pad = round_up(longitudes, LANES)
    long_tiles = long_pad // LANES
    tiles = round_up(tile_count + long_tiles, LANES)
    sent_tiles = tile_count
    group_rows = levels * lat_band // half_size
    pieces = 2 * KW // PIECE
    chunks = block_count // CHUNK
    fine = np.stack(cos_sin(np.arange(STEP)))
    coarse = np.stack(cos_sin(STEP * np.arange(long_pad // STEP)), axis=1)
    start = np.stack(cos_sin(longitudes * np.arange(cols)), axis=1)
    width = width_of(mesh)
    places = np.arange(half_size)
    mirrored = (half_size // width - 1 - places // width) * width + places % width
    away = np.concatenate([half_size + mirrored - places, mirrored - places - half_size])
    turn = np.stack(cos_sin(longitudes * away % NLON), axis=1)

    slab_rows = levels * capacity
    smem = pl.BlockSpec(memory_space=pltpu.SMEM)
    vmem = pl.BlockSpec(memory_space=pltpu.VMEM)
    anywhere = pl.BlockSpec(memory_space=pl.ANY)
    shape = jax.ShapeDtypeStruct((levels, lat_band, longitudes), F32)
    dma = pltpu.SemaphoreType.DMA
    results = pl.pallas_call(
        functools.partial(
            remap_kernel, bands, cols, width, levels, capacity, KW, NLON, longitudes, sent_tiles
        ),
        out_shape=(pltpu.VMEM(shape.shape, F32), pltpu.VMEM(shape.shape, F32)),
        in_specs=[smem] * 2 + [vmem] * 7 + [anywhere],
        out_specs=(vmem, vmem),
        scratch_shapes=[
            pltpu.VMEM(weights.shape, BF16),
            pltpu.VMEM((source.shape[1] // LANES, 16, LANES), BF16),
            pltpu.VMEM((source.shape[1] // LANES, 16, LANES), BF16),
            pltpu.VMEM((block_count, 8, LANES), F32),
            pltpu.VMEM((levels, tiles, LANES), F32),
            pltpu.VMEM((long_pad, 2 * KW), BF16),
            pltpu.VMEM((long_pad, 2 * KW), BF16),
            pltpu.VMEM((2, STEP, KW), F32),
            pltpu.VMEM((2, long_tiles, levels * lat_band, LANES), F32),
            pltpu.VMEM((3 * cols, slab_rows, LANES), F32),
            pltpu.VMEM((3 * half_size, slab_rows, LANES), F32),
            pltpu.VMEM((3 * half_size, slab_rows, LANES), F32),
            pltpu.VMEM((levels, tiles, LANES), F32),
            pltpu.VMEM((levels, sent_tiles, LANES), F32),
            pltpu.VMEM((3 * half_size, 2, LANES), F32),
            pltpu.VMEM((3 * half_size, 2, LANES), F32),
            pltpu.VMEM((lat_here, LANES), jnp.int32),
            pltpu.VMEM((lat_here, LANES), jnp.int32),
            pltpu.VMEM((half_size, group_rows, 2 * KW), F32),
            pltpu.VMEM((half_size, group_rows, 2 * KW), F32),
            pltpu.VMEM((group_rows, 2 * KW), F32),
            pltpu.VMEM((group_rows, 2 * KW), F32),
            pltpu.VMEM((group_rows, 2 * KW), F32),
            pltpu.VMEM((half_size, group_rows, 2 * KW), F32),
            dma((chunks,)),
            dma((3,)),
            dma((3,)),
            dma,
            dma,
            dma((3,)),
            dma((3,)),
            dma((3,)),
            dma,
            dma,
            dma((pieces,)),
            dma((pieces,)),
            dma((pieces,)),
            dma((pieces,)),
            dma((pieces,)),
            dma((pieces,)),
        ],
        compiler_params=pltpu.CompilerParams(
            collective_id=0, has_side_effects=True, vmem_limit_bytes=48 << 20
        ),
    )(
        *(
            pltpu.with_memory_space_constraint(operand, pltpu.HBM)
            for operand in (
                cutoff,
                source_block,
                owner_device.reshape(1, block_count),
                target_tile.reshape(1, block_count),
                jnp.asarray(fine),
                jnp.asarray(coarse),
                jnp.asarray(start),
                jnp.asarray(turn),
                source,
                weights,
            )
        )
    )
    return pl.pallas_call(
        deliver,
        out_shape=(shape, shape),
        in_specs=[vmem] * 2,
        out_specs=(anywhere, anywhere),
        scratch_shapes=[dma((2,))],
    )(*(pltpu.with_memory_space_constraint(result, pltpu.VMEM) for result in results))


def solution(mesh):
    in_specs = (
        P(None, ("band", "col")),
        P(("band", "col"), None, None),
        P(("band", "col")),
        P(("band", "col"), None),
        P(("band", "col")),
        P(("band", "col")),
    )
    out_specs = (P(None, "band", "col"), P(None, "band", "col"))
    return jax.shard_map(
        functools.partial(local, mesh),
        mesh=mesh,
        in_specs=in_specs,
        out_specs=out_specs,
        check_vma=False,
    )
```

```python
import functools

import jax
import jax.numpy as jnp
import numpy as np
from jax import lax
from jax.experimental import pallas as pl
from jax.experimental.pallas import tpu as pltpu
from jax.sharding import PartitionSpec as P

NLON = 7200
KW = 512
LANES = 128
STEP = 16
CHUNK = 32
PIECE = 256
TOGETHER = 4
EARLY = 2
BETWEEN = 1
DENSE = (0, 4, 4, 4, 5, 6)
MESH = pl.DeviceIdType.MESH
F32 = jnp.float32
BF16 = jnp.bfloat16


def round_up(value, multiple):
    return (value + multiple - 1) // multiple * multiple


def split(value):
    high = value.astype(BF16)
    return high, (value - high.astype(F32)).astype(BF16)


def dot(left, right, left_dim=1, right_dim=0):
    return lax.dot_general(
        left, right, (((left_dim,), (right_dim,)), ((), ())), preferred_element_type=F32
    )


def remap_kernel(
    bands, cols, width, levels, capacity, wave_count, period, longitudes, tile_count,
    cutoff_in, block_in, owner_in, tile_in, source_in, fine_in, coarse_in, start_in, turn_in, weights,
    remapped, filtered,
    cutoff, source_block, owner_row, tile_row, source, fine, coarse, start, turn,
    weight_buf, source_even, source_odd, partial,
    sums, table_high, table_low, rotated, field, slab, recv, relay, relay_sums, passed,
    tags_out, tags_in, cut_out, cut_in,
    spectra, arrived, half_sum, other_sum, scaled, gathered,
    weight_sem, tag_send, tag_recv, cut_send, cut_recv,
    send_sem, recv_sem, relay_sem, pass_send, pass_recv,
    scatter_send, scatter_recv, cross_send, cross_recv, spread_send, spread_recv, operand_sem,
):
    band, col = lax.axis_index("band"), lax.axis_index("col")
    blocks = weights.shape[0]
    rows = levels * capacity
    half_size = cols // 2
    half, place_in_half = col // half_size, lax.rem(col, half_size)
    layers = half_size // width
    layer = place_in_half // width

    def mirror(where):
        return (layers - 1 - where // width) * width + where % width

    def group_of(where):
        return jnp.where(half == 0, where, mirror(where))

    counterpart = (band, (1 - half) * half_size + mirror(place_in_half))

    def valid(offset):
        target = band + (offset - 1)
        return (target >= 0) & (target < bands)

    weight_copies = [
        pltpu.make_async_copy(
            weights.at[pl.ds(first, CHUNK)], weight_buf.at[pl.ds(first, CHUNK)], weight_sem.at[i]
        )
        for i, first in enumerate(range(0, blocks, CHUNK))
    ]
    operand_copies = [
        pltpu.make_async_copy(there, here, operand_sem.at[i])
        for i, (there, here) in enumerate(
            (
                (owner_in, owner_row),
                (tile_in, tile_row),
                (block_in, source_block),
                (source_in, source),
                (cutoff_in, cutoff),
                (fine_in, fine),
                (coarse_in, coarse),
                (start_in, start),
                (turn_in, turn),
            )
        )
    ]
    for copy in operand_copies[:5] + weight_copies[:EARLY]:
        copy.start()

    barrier = pltpu.get_barrier_semaphore()

    def greet(device):
        pl.semaphore_signal(barrier, inc=1, device_id=device, device_id_type=MESH)

    def greet_half(offset):
        def one(to, carry):
            def signal():
                greet((band + (offset - 1), half * half_size + to))

            if offset == 1:
                pl.when(to != place_in_half)(signal)
            else:
                signal()
            return carry

        lax.fori_loop(0, half_size, one, 0, unroll=half_size <= 4)

    for offset in (0, 2, 1):
        pl.when(valid(offset))(functools.partial(greet_half, offset))
    greet(counterpart)

    for copy in operand_copies[:3]:
        copy.wait()
    for copy in weight_copies[EARLY:] + operand_copies[5:]:
        copy.start()
    owners = owner_row[...]
    sublane = lax.broadcasted_iota(jnp.int32, (blocks, blocks), 0)
    lane = lax.broadcasted_iota(jnp.int32, (blocks, blocks), 1)
    owners_wide = jnp.broadcast_to(owners.astype(F32), (8, blocks))
    owner_column = jnp.transpose(owners_wide)[:, 0:1]
    earlier = (owner_column == owners.astype(F32)) & (sublane < lane)
    rank = jnp.sum(earlier.astype(jnp.int32), axis=0, keepdims=True)
    place = owners - (band - 1) * cols
    slot = place * capacity + rank
    slot_lane = lax.broadcasted_iota(jnp.int32, (LANES, blocks), 0)
    tile_at = jnp.where(slot_lane == rank, tile_row[...], 0).astype(F32).astype(BF16)
    place_ids = lax.broadcasted_iota(jnp.int32, (3 * cols, blocks), 0)
    chosen = (place_ids == place).astype(F32).astype(BF16)
    tags = dot(chosen, tile_at, 1, 1)
    for offset in range(3):
        for to in range(half_size):
            here = [
                tags[row : row + 1]
                for row in (
                    offset * cols + lat_half * half_size + where
                    for where in (to, mirror(to))
                    for lat_half in range(2)
                )
            ]
            tags_out[offset * half_size + to, 0:1] = jnp.where(half == 0, here[0], here[1])
            tags_out[offset * half_size + to, 1:2] = jnp.where(half == 0, here[3], here[2])
    lat_here = cutoff.shape[0]
    for copy in operand_copies[3:5]:
        copy.wait()
    for lat in range(lat_here):
        cut_out[lat : lat + 1] = jnp.full((1, LANES), cutoff[lat], jnp.int32)

    above = jnp.zeros((16 - levels, LANES), BF16)
    below = jnp.zeros((8, LANES), BF16)
    for index in range(source_even.shape[0]):
        value = source[:, index * LANES : (index + 1) * LANES]
        source_even[index] = jnp.concatenate([value, above], axis=0)
        source_odd[index] = jnp.concatenate([below, value, above[: 8 - levels]], axis=0)

    for i, copy in enumerate(weight_copies):
        copy.wait()
        for index in range(i * CHUNK, (i + 1) * CHUNK, 2):
            left = jnp.concatenate(
                [source_even[source_block[index]], source_odd[source_block[index + 1]]], axis=1
            )
            right = weight_buf[index : index + 2].reshape(2 * LANES, LANES)
            partial[index : index + 2] = dot(left, right).reshape(2, 8, LANES)

    data = jnp.concatenate([partial[:, level, :] for level in range(levels)], axis=1)
    stacked = jnp.concatenate(split(data), axis=0)

    def fill(offset):
        group = cols * capacity
        ids = lax.broadcasted_iota(jnp.int32, (group, blocks), 0) + offset * group
        placing = (ids == slot).astype(F32).astype(BF16)
        placed = dot(jnp.concatenate([placing, placing], axis=1), stacked)
        here = pl.ds(offset * cols, cols)
        for level in range(levels):
            piece = placed[:, level * LANES : (level + 1) * LANES]
            slab[here, level * capacity : (level + 1) * capacity, :] = piece.reshape(
                cols, capacity, LANES
            )

    pl.when(valid(0))(functools.partial(fill, 0))
    pl.when(band == 0)(functools.partial(fill, 2))

    inner_band = (band > 0) & (band < bands - 1)
    neighbours = jnp.where(inner_band, 2, 1) if bands > 1 else 0
    pl.semaphore_wait(barrier, half_size * (1 + neighbours))

    def send_to_half(source_of, target, sems_out, sems_in, offset):
        def one(step, carry):
            to = lax.rem(place_in_half + half_size // 2 + step, half_size)

            def start_remote():
                pltpu.make_async_remote_copy(
                    src_ref=source_of(to),
                    dst_ref=target,
                    send_sem=sems_out.at[offset],
                    recv_sem=sems_in.at[2 - offset],
                    device_id=(band + (offset - 1), half * half_size + to),
                    device_id_type=MESH,
                ).start()

            if offset == 1:
                pl.when(to != place_in_half)(start_remote)
            else:
                start_remote()
            return carry

        lax.fori_loop(0, half_size, one, 0, unroll=half_size <= 4)
        if offset == 1:
            pltpu.make_async_copy(source_of(place_in_half), target, sems_in.at[1]).start()

    def push_tags(offset):
        send_to_half(
            lambda to: tags_out.at[offset * half_size + to],
            tags_in.at[(2 - offset) * half_size + place_in_half],
            tag_send, tag_recv, offset,
        )

    def push(owner_half, owner_of, into, sems, offset):
        send_to_half(
            lambda to: slab.at[offset * cols + owner_half * half_size + owner_of(to)],
            into.at[(2 - offset) * half_size + place_in_half],
            send_sem, sems, offset,
        )

    cut_copy = pltpu.make_async_remote_copy(
        src_ref=cut_out,
        dst_ref=cut_in,
        send_sem=cut_send,
        recv_sem=cut_recv,
        device_id=counterpart,
        device_id_type=MESH,
    )

    def place_and_push(offset):
        if offset == 1:
            fill(offset)
        elif offset == 2:
            pl.when(band > 0)(functools.partial(fill, offset))
        push(1 - half, mirror, relay, relay_sem, offset)

    pl.when(valid(0))(functools.partial(place_and_push, 0))
    pl.when(band == 0)(functools.partial(place_and_push, 2))
    for offset in (0, 2, 1):
        pl.when(valid(offset))(functools.partial(push_tags, offset))
    cut_copy.start()
    pl.when((band > 0) & valid(2))(functools.partial(place_and_push, 2))
    place_and_push(1)
    for offset in (0, 2, 1):
        pl.when(valid(offset))(functools.partial(push, half, lambda to: to, recv, recv_sem, offset))

    for copy in operand_copies[5:]:
        copy.wait()
    begin = start[col]
    cos_start, sin_start = begin[0:1], begin[1:2]
    rotated[0] = fine[0] * cos_start - fine[1] * sin_start
    rotated[1] = fine[1] * cos_start + fine[0] * sin_start

    def table_step(step, carry):
        pair = coarse[step]
        cos_base, sin_base = pair[0:1], pair[1:2]
        cos_fine, sin_fine = rotated[0], rotated[1]
        at = pl.ds(pl.multiple_of(step * STEP, STEP), STEP)
        for first, value in (
            (0, cos_base * cos_fine - sin_base * sin_fine),
            (wave_count, sin_base * cos_fine + cos_base * sin_fine),
        ):
            high, low = split(value)
            table_high[at, first : first + wave_count] = high
            table_low[at, first : first + wave_count] = low
        return carry

    lax.fori_loop(0, coarse.shape[0], table_step, 0)

    tiles = sums.shape[1]
    sums[...] = jnp.zeros_like(sums)
    relay_sums[...] = jnp.zeros_like(relay_sums)

    def wait_tags(offset):
        here = tags_in.at[pl.ds(offset * half_size, half_size)]
        pltpu.make_async_copy(here, here, tag_recv.at[offset]).wait()

    for offset in (0, 2, 1):
        pl.when(valid(offset))(functools.partial(wait_tags, offset))

    def receive(ref, sems, into, kind, offset):
        here = pl.ds(offset * half_size, half_size)
        tag_rows = [
            tags_in[offset * half_size + sender, kind : kind + 1] for sender in range(half_size)
        ]
        tags = jnp.transpose(jnp.concatenate(tag_rows * (-(-8 // half_size)), axis=0))
        wide = lax.broadcasted_iota(jnp.int32, (capacity, tiles), 1).astype(F32)
        chooser = jnp.concatenate(
            [
                (tags[:capacity, sender : sender + 1] == wide).astype(F32)
                for sender in range(half_size)
            ],
            axis=0,
        )
        chooser = jnp.transpose(chooser).astype(BF16)
        pltpu.make_async_copy(ref.at[here], ref.at[here], sems.at[offset]).wait()
        incoming = jnp.concatenate(
            [
                ref[here, level * capacity : (level + 1) * capacity, :].reshape(
                    half_size * capacity, LANES
                )
                for level in range(levels)
            ],
            axis=1,
        )
        high, low = split(incoming)
        total = dot(chooser, high) + dot(chooser, low)
        for level in range(levels):
            into[level] += total[:, level * LANES : (level + 1) * LANES]

    def dense_start(first, count):
        here = (pl.ds(first, count), pl.ds(0, tile_count))
        pltpu.make_async_remote_copy(
            src_ref=relay_sums.at[here],
            dst_ref=passed.at[pl.ds(first, count)],
            send_sem=pass_send,
            recv_sem=pass_recv,
            device_id=counterpart,
            device_id_type=MESH,
        ).start()

    inner = jnp.where(half == 0, layer >= layers // 2, layer < layers - layers // 2)
    outer = jnp.logical_not(inner)
    ends = [levels * share // DENSE[-1] for share in DENSE]

    def dense_part(index):
        if ends[index + 1] > ends[index]:
            pl.when(outer)(
                functools.partial(dense_start, ends[index], ends[index + 1] - ends[index])
            )

    for offset in (0, 2, 1):
        pl.when(valid(offset))(functools.partial(receive, relay, relay_sem, relay_sums, 1, offset))
    pl.when(inner)(functools.partial(dense_start, 0, levels))
    dense_part(0)

    long_tiles, field_rows = field.shape[1:3]
    lat_band = field_rows // levels
    group_rows = field_rows // half_size
    shape3 = (levels, long_tiles, LANES)
    lane3 = lax.broadcasted_iota(jnp.int32, shape3, 2)
    inside = lax.broadcasted_iota(jnp.int32, shape3, 1) * LANES + lane3 < longitudes

    def row_of(level, lat):
        owner, within = divmod(lat, lat_here)
        lat_half, owner_place = divmod(owner, half_size)
        group = mirror(owner_place) if lat_half else owner_place
        return group * group_rows + (level * 2 + lat_half) * lat_here + within

    def lat_rows(ref, lat):
        first, shift = divmod(lat * longitudes, LANES)
        value = ref[:, first : first + long_tiles, :]
        if shift:
            after = ref[:, first + 1 : first + 1 + long_tiles, :]
            value = jnp.where(
                lane3 < LANES - shift,
                pltpu.roll(value, LANES - shift, 2),
                pltpu.roll(after, LANES - shift, 2),
            )
        return jnp.where(inside, value, 0.0)

    def rows_of_field(ref, index):
        for lat in range(lat_band):
            value = lat_rows(ref, lat)
            for level in range(levels):
                field[index, :, row_of(level, lat), :] = value[level]
        rows_wide = jnp.concatenate([field[index, tile] for tile in range(long_tiles)], axis=1)
        high, low = split(rows_wide)
        return jnp.concatenate([high, low], axis=0), high

    def transformed(parts, waves):
        both = dot(parts[0], table_high[:, waves])
        return both[:field_rows] + both[field_rows:] + dot(parts[1], table_low[:, waves])

    relayed = transformed(rows_of_field(relay_sums, 1), slice(None))
    angle = turn[col]
    cos_part, sin_part = relayed[:, :wave_count], relayed[:, wave_count:]
    grouped = (half_size, group_rows, wave_count)
    spectra[:, :, :wave_count] = (cos_part * angle[0:1] - sin_part * angle[1:2]).reshape(grouped)
    spectra[:, :, wave_count:] = (sin_part * angle[0:1] + cos_part * angle[1:2]).reshape(grouped)

    for offset in (0, 2, 1):
        pl.when(valid(offset))(functools.partial(receive, recv, recv_sem, sums, 0, offset))

    waves = 2 * wave_count
    pieces = [slice(first, first + PIECE) for first in range(0, waves, PIECE)]

    def to_half(source_of, target, sem_out, sem_in):
        def one(step, carry):
            to = lax.rem(place_in_half + half_size // 2 + step, half_size)

            def start_remote():
                pltpu.make_async_remote_copy(
                    src_ref=source_of(to),
                    dst_ref=target,
                    send_sem=sem_out,
                    recv_sem=sem_in,
                    device_id=(band, half * half_size + to),
                    device_id_type=MESH,
                ).start()

            pl.when(to != place_in_half)(start_remote)
            return carry

        lax.fori_loop(0, half_size, one, 0, unroll=half_size <= 4)
        pltpu.make_async_copy(source_of(place_in_half), target, sem_in).start()

    parts = rows_of_field(sums, 0)
    for i, piece in enumerate(pieces):
        if i % TOGETHER == 0:
            wide = slice(piece.start, piece.start + TOGETHER * PIECE)
            spectra[:, :, wide] += transformed(parts, wide).reshape(
                half_size, group_rows, TOGETHER * PIECE
            )
        to_half(
            lambda to: spectra.at[group_of(to), :, piece],
            arrived.at[place_in_half, :, piece],
            scatter_send.at[i], scatter_recv.at[i],
        )
    dense_part(1)

    cut_copy.wait()
    cuts = []
    for lat_half in range(2):
        for lat in range(lat_here):
            cuts.append(
                jnp.where(half == lat_half, cut_out[lat : lat + 1], cut_in[lat : lat + 1])
            )
    cut_rows = jnp.concatenate(cuts * (group_rows // len(cuts)), axis=0)

    def gain_of(tile):
        j = lax.broadcasted_iota(jnp.int32, (group_rows, LANES), 1) + tile * LANES
        wave = jnp.where(j >= wave_count, j - wave_count, j)
        weight = jnp.where(wave == 0, 1.0, 2.0) / period
        return jnp.where(wave <= cut_rows, weight, 0.0).astype(F32)

    gains = jnp.concatenate([gain_of(tile) for tile in range(waves // LANES)], axis=1)

    def cross(i):
        return pltpu.make_async_remote_copy(
            src_ref=half_sum.at[:, pieces[i]],
            dst_ref=other_sum.at[:, pieces[i]],
            send_sem=cross_send.at[i],
            recv_sem=cross_recv.at[i],
            device_id=counterpart,
            device_id_type=MESH,
        )

    for i, piece in enumerate(pieces):
        here = arrived.at[:, :, piece]
        pltpu.make_async_copy(here, here, scatter_recv.at[i]).wait()
        total = arrived[0, :, piece]
        for sender in range(1, half_size):
            total += arrived[sender, :, piece]
        half_sum[:, piece] = total
        cross(i).start()
    dense_part(2)
    for i, piece in enumerate(pieces):
        cross(i).wait_recv()
        scaled[:, piece] = (half_sum[:, piece] + other_sum[:, piece]) * gains[:, piece]
        to_half(
            lambda to: scaled.at[:, piece],
            gathered.at[group_of(place_in_half), :, piece],
            spread_send.at[i], spread_recv.at[i],
        )
        if i == BETWEEN:
            dense_part(3)
    dense_part(4)

    def drain(offset):
        sent = slab.at[pl.ds(0, cols - 2 if offset == 1 else cols)]
        pltpu.make_async_copy(sent, sent, send_sem.at[offset]).wait()
        tag = tags_out.at[pl.ds(0, half_size - 1 if offset == 1 else half_size)]
        pltpu.make_async_copy(tag, tag, tag_send.at[offset]).wait()

    for offset in range(3):
        pl.when(valid(offset))(functools.partial(drain, offset))
    for i, piece in enumerate(pieces):
        others = arrived.at[pl.ds(0, half_size - 1), :, piece]
        pltpu.make_async_copy(others, others, scatter_send.at[i]).wait()
        cross(i).wait_send()

    def natural(spread):
        rows_of = [
            spread[row : row + lat_here]
            for level in range(levels)
            for row in (row_of(level, lat) for lat in range(0, lat_band, lat_here))
        ]
        return jnp.concatenate(rows_of, axis=0)[:, :longitudes].reshape(
            levels, lat_band, longitudes
        )

    result = None
    for i, piece in enumerate(pieces):
        here = gathered.at[:, :, piece]
        pltpu.make_async_copy(here, here, spread_recv.at[i]).wait()
        high, low = split(gathered[:, :, piece].reshape(field_rows, PIECE))
        both = dot(jnp.concatenate([high, low], axis=0), table_high[:, piece], 1, 1)
        added = both[:field_rows] + both[field_rows:] + dot(high, table_low[:, piece], 1, 1)
        result = added if result is None else result + added
    filtered[...] = natural(result)

    pltpu.make_async_copy(passed, passed, pass_recv).wait()
    sums[:, :tile_count, :] += passed[...]
    for lat in range(lat_band):
        value = lat_rows(sums, lat)
        for level in range(levels):
            field[0, :, level * lat_band + lat, :] = value[level]
    rows_wide = jnp.concatenate([field[0, tile] for tile in range(long_tiles)], axis=1)
    remapped[...] = rows_wide[:, :longitudes].reshape(levels, lat_band, longitudes)

    pltpu.make_async_copy(passed, passed, pass_send).wait()
    for i, piece in enumerate(pieces):
        others = arrived.at[pl.ds(0, half_size - 1), :, piece]
        pltpu.make_async_copy(others, others, spread_send.at[i]).wait()


def deliver(first, second, first_out, second_out, sem):
    copies = [
        pltpu.make_async_copy(first, first_out, sem.at[0]),
        pltpu.make_async_copy(second, second_out, sem.at[1]),
    ]
    for copy in copies:
        copy.start()
    for copy in copies:
        copy.wait()


def cos_sin(positions):
    phases = positions[:, None] * np.arange(KW)[None, :] % NLON
    angles = phases * (2 * np.pi / NLON)
    return np.cos(angles).astype(np.float32), np.sin(angles).astype(np.float32)


def width_of(mesh):
    cols = mesh.shape["col"]
    places = [getattr(device, "coords", None) for device in mesh.devices[0]]
    if None in places:
        return 1
    width = sum(place[2] == places[0][2] for place in places)
    return width if cols % (2 * width) == 0 else 1


def local(mesh, source, weights, source_block, owner_device, target_tile, cutoff):
    bands, cols = mesh.shape["band"], mesh.shape["col"]
    levels = source.shape[0]
    block_count, block_width = weights.shape[:2]
    lat_here = cutoff.shape[0]
    lat_band = lat_here * cols
    half_size = cols // 2
    longitudes = NLON // cols
    cell_count = lat_band * longitudes
    tile_count = (cell_count + block_width - 1) // block_width
    regular = (tile_count + cols - 1) // cols
    capacity = regular + max(1, (block_count - cols * regular + 2 * cols - 1) // (2 * cols))
    capacity = round_up(capacity, 8)
    long_pad = round_up(longitudes, LANES)
    long_tiles = long_pad // LANES
    tiles = round_up(tile_count + long_tiles, LANES)
    sent_tiles = tile_count
    group_rows = levels * lat_band // half_size
    pieces = 2 * KW // PIECE
    chunks = block_count // CHUNK
    fine = np.stack(cos_sin(np.arange(STEP)))
    coarse = np.stack(cos_sin(STEP * np.arange(long_pad // STEP)), axis=1)
    start = np.stack(cos_sin(longitudes * np.arange(cols)), axis=1)
    width = width_of(mesh)
    places = np.arange(half_size)
    mirrored = (half_size // width - 1 - places // width) * width + places % width
    away = np.concatenate([half_size + mirrored - places, mirrored - places - half_size])
    turn = np.stack(cos_sin(longitudes * away % NLON), axis=1)

    slab_rows = levels * capacity
    vmem = pl.BlockSpec(memory_space=pltpu.VMEM)
    anywhere = pl.BlockSpec(memory_space=pl.ANY)
    shape = jax.ShapeDtypeStruct((levels, lat_band, longitudes), F32)
    dma = pltpu.SemaphoreType.DMA
    results = pl.pallas_call(
        functools.partial(
            remap_kernel, bands, cols, width, levels, capacity, KW, NLON, longitudes, sent_tiles
        ),
        out_shape=(pltpu.VMEM(shape.shape, F32), pltpu.VMEM(shape.shape, F32)),
        in_specs=[anywhere] * 10,
        out_specs=(vmem, vmem),
        scratch_shapes=[
            pltpu.SMEM(cutoff.shape, jnp.int32),
            pltpu.SMEM(source_block.shape, jnp.int32),
            pltpu.VMEM((1, block_count), jnp.int32),
            pltpu.VMEM((1, block_count), jnp.int32),
            pltpu.VMEM(source.shape, BF16),
            pltpu.VMEM(fine.shape, F32),
            pltpu.VMEM(coarse.shape, F32),
            pltpu.VMEM(start.shape, F32),
            pltpu.VMEM(turn.shape, F32),
            pltpu.VMEM(weights.shape, BF16),
            pltpu.VMEM((source.shape[1] // LANES, 16, LANES), BF16),
            pltpu.VMEM((source.shape[1] // LANES, 16, LANES), BF16),
            pltpu.VMEM((block_count, 8, LANES), F32),
            pltpu.VMEM((levels, tiles, LANES), F32),
            pltpu.VMEM((long_pad, 2 * KW), BF16),
            pltpu.VMEM((long_pad, 2 * KW), BF16),
            pltpu.VMEM((2, STEP, KW), F32),
            pltpu.VMEM((2, long_tiles, levels * lat_band, LANES), F32),
            pltpu.VMEM((3 * cols, slab_rows, LANES), F32),
            pltpu.VMEM((3 * half_size, slab_rows, LANES), F32),
            pltpu.VMEM((3 * half_size, slab_rows, LANES), F32),
            pltpu.VMEM((levels, tiles, LANES), F32),
            pltpu.VMEM((levels, sent_tiles, LANES), F32),
            pltpu.VMEM((3 * half_size, 2, LANES), F32),
            pltpu.VMEM((3 * half_size, 2, LANES), F32),
            pltpu.VMEM((lat_here, LANES), jnp.int32),
            pltpu.VMEM((lat_here, LANES), jnp.int32),
            pltpu.VMEM((half_size, group_rows, 2 * KW), F32),
            pltpu.VMEM((half_size, group_rows, 2 * KW), F32),
            pltpu.VMEM((group_rows, 2 * KW), F32),
            pltpu.VMEM((group_rows, 2 * KW), F32),
            pltpu.VMEM((group_rows, 2 * KW), F32),
            pltpu.VMEM((half_size, group_rows, 2 * KW), F32),
            dma((chunks,)),
            dma((3,)),
            dma((3,)),
            dma,
            dma,
            dma((3,)),
            dma((3,)),
            dma((3,)),
            dma,
            dma,
            dma((pieces,)),
            dma((pieces,)),
            dma((pieces,)),
            dma((pieces,)),
            dma((pieces,)),
            dma((pieces,)),
            dma((9,)),
        ],
        compiler_params=pltpu.CompilerParams(
            collective_id=0, has_side_effects=True, vmem_limit_bytes=48 << 20
        ),
    )(
        *(
            pltpu.with_memory_space_constraint(operand, pltpu.HBM)
            for operand in (
                cutoff,
                source_block,
                owner_device.reshape(1, block_count),
                target_tile.reshape(1, block_count),
                source,
                jnp.asarray(fine),
                jnp.asarray(coarse),
                jnp.asarray(start),
                jnp.asarray(turn),
                weights,
            )
        )
    )
    return pl.pallas_call(
        deliver,
        out_shape=(shape, shape),
        in_specs=[vmem] * 2,
        out_specs=(anywhere, anywhere),
        scratch_shapes=[dma((2,))],
    )(*(pltpu.with_memory_space_constraint(result, pltpu.VMEM) for result in results))


def solution(mesh):
    in_specs = (
        P(None, ("band", "col")),
        P(("band", "col"), None, None),
        P(("band", "col")),
        P(("band", "col"), None),
        P(("band", "col")),
        P(("band", "col")),
    )
    out_specs = (P(None, "band", "col"), P(None, "band", "col"))
    return jax.shard_map(
        functools.partial(local, mesh),
        mesh=mesh,
        in_specs=in_specs,
        out_specs=out_specs,
        check_vma=False,
    )
```

```python
import functools

import jax
import jax.numpy as jnp
import numpy as np
from jax import lax
from jax.experimental import pallas as pl
from jax.experimental.pallas import tpu as pltpu
from jax.sharding import PartitionSpec as P

NLON = 7200
KW = 512
LANES = 128
STEP = 16
CHUNK = 32
PIECE = 256
TOGETHER = 4
EARLY = 2
BETWEEN = 1
DENSE = (0, 4, 4, 4, 5, 6)
MESH = pl.DeviceIdType.MESH
F32 = jnp.float32
BF16 = jnp.bfloat16


def round_up(value, multiple):
    return (value + multiple - 1) // multiple * multiple


def split(value):
    high = value.astype(BF16)
    return high, (value - high.astype(F32)).astype(BF16)


def dot(left, right, left_dim=1, right_dim=0):
    return lax.dot_general(
        left, right, (((left_dim,), (right_dim,)), ((), ())), preferred_element_type=F32
    )


def remap_kernel(
    bands, cols, width, levels, capacity, wave_count, period, longitudes, tile_count,
    cutoff_in, block_in, owner_in, tile_in, source_in, fine_in, coarse_in, start_in, turn_in, weights,
    remapped, filtered,
    cutoff, source_block, owner_row, tile_row, source, fine, coarse, start, turn,
    weight_buf, source_even, source_odd, partial, stacked,
    sums, table_high, table_low, rotated, field, slab, recv, relay, relay_sums, passed,
    tags_out, tags_in, cut_out, cut_in,
    spectra, arrived, half_sum, other_sum, scaled, gathered,
    weight_sem, tag_send, tag_recv, cut_send, cut_recv,
    send_sem, recv_sem, relay_sem, pass_send, pass_recv,
    scatter_send, scatter_recv, cross_send, cross_recv, spread_send, spread_recv, operand_sem,
):
    band, col = lax.axis_index("band"), lax.axis_index("col")
    blocks = weights.shape[0]
    rows = levels * capacity
    half_size = cols // 2
    half, place_in_half = col // half_size, lax.rem(col, half_size)
    layers = half_size // width
    layer = place_in_half // width

    def mirror(where):
        return (layers - 1 - where // width) * width + where % width

    def group_of(where):
        return jnp.where(half == 0, where, mirror(where))

    counterpart = (band, (1 - half) * half_size + mirror(place_in_half))

    def valid(offset):
        target = band + (offset - 1)
        return (target >= 0) & (target < bands)

    weight_copies = [
        pltpu.make_async_copy(
            weights.at[pl.ds(first, CHUNK)], weight_buf.at[pl.ds(first, CHUNK)], weight_sem.at[i]
        )
        for i, first in enumerate(range(0, blocks, CHUNK))
    ]
    operand_copies = [
        pltpu.make_async_copy(there, here, operand_sem.at[i])
        for i, (there, here) in enumerate(
            (
                (owner_in, owner_row),
                (tile_in, tile_row),
                (block_in, source_block),
                (source_in, source),
                (cutoff_in, cutoff),
                (fine_in, fine),
                (coarse_in, coarse),
                (start_in, start),
                (turn_in, turn),
            )
        )
    ]
    for copy in operand_copies[:5] + weight_copies[:EARLY]:
        copy.start()

    barrier = pltpu.get_barrier_semaphore()

    def greet(device):
        pl.semaphore_signal(barrier, inc=1, device_id=device, device_id_type=MESH)

    def greet_half(offset):
        def one(to, carry):
            def signal():
                greet((band + (offset - 1), half * half_size + to))

            if offset == 1:
                pl.when(to != place_in_half)(signal)
            else:
                signal()
            return carry

        lax.fori_loop(0, half_size, one, 0, unroll=half_size <= 4)

    for offset in (0, 2, 1):
        pl.when(valid(offset))(functools.partial(greet_half, offset))
    greet(counterpart)

    for copy in operand_copies[:3]:
        copy.wait()
    for copy in weight_copies[EARLY:] + operand_copies[5:]:
        copy.start()
    owners = owner_row[...]
    sublane = lax.broadcasted_iota(jnp.int32, (blocks, blocks), 0)
    lane = lax.broadcasted_iota(jnp.int32, (blocks, blocks), 1)
    owners_wide = jnp.broadcast_to(owners.astype(F32), (8, blocks))
    owner_column = jnp.transpose(owners_wide)[:, 0:1]
    earlier = (owner_column == owners.astype(F32)) & (sublane < lane)
    rank = jnp.sum(earlier.astype(jnp.int32), axis=0, keepdims=True)
    place = owners - (band - 1) * cols
    slot = place * capacity + rank
    slot_lane = lax.broadcasted_iota(jnp.int32, (LANES, blocks), 0)
    tile_at = jnp.where(slot_lane == rank, tile_row[...], 0).astype(F32).astype(BF16)
    place_ids = lax.broadcasted_iota(jnp.int32, (3 * cols, blocks), 0)
    chosen = (place_ids == place).astype(F32).astype(BF16)
    tags = dot(chosen, tile_at, 1, 1)
    for offset in range(3):
        for to in range(half_size):
            here = [
                tags[row : row + 1]
                for row in (
                    offset * cols + lat_half * half_size + where
                    for where in (to, mirror(to))
                    for lat_half in range(2)
                )
            ]
            tags_out[offset * half_size + to, 0:1] = jnp.where(half == 0, here[0], here[1])
            tags_out[offset * half_size + to, 1:2] = jnp.where(half == 0, here[3], here[2])
    lat_here = cutoff.shape[0]
    for copy in operand_copies[3:5]:
        copy.wait()
    for lat in range(lat_here):
        cut_out[lat : lat + 1] = jnp.full((1, LANES), cutoff[lat], jnp.int32)

    above = jnp.zeros((16 - levels, LANES), BF16)
    below = jnp.zeros((8, LANES), BF16)
    for index in range(source_even.shape[0]):
        value = source[:, index * LANES : (index + 1) * LANES]
        source_even[index] = jnp.concatenate([value, above], axis=0)
        source_odd[index] = jnp.concatenate([below, value, above[: 8 - levels]], axis=0)

    def pack(i):
        here = slice(i * CHUNK, (i + 1) * CHUNK)
        for level in range(levels):
            high, low = split(partial[here, level, :])
            columns = slice(level * LANES, (level + 1) * LANES)
            stacked[here, columns] = high
            stacked[blocks + here.start : blocks + here.stop, columns] = low

    for i, copy in enumerate(weight_copies):
        copy.wait()
        if i:
            pack(i - 1)
        for index in range(i * CHUNK, (i + 1) * CHUNK, 2):
            left = jnp.concatenate(
                [source_even[source_block[index]], source_odd[source_block[index + 1]]], axis=1
            )
            right = weight_buf[index : index + 2].reshape(2 * LANES, LANES)
            partial[index : index + 2] = dot(left, right).reshape(2, 8, LANES)

    pack(len(weight_copies) - 1)

    def fill(offset):
        group = cols * capacity
        ids = lax.broadcasted_iota(jnp.int32, (group, blocks), 0) + offset * group
        placing = (ids == slot).astype(F32).astype(BF16)
        placed = dot(jnp.concatenate([placing, placing], axis=1), stacked[...])
        here = pl.ds(offset * cols, cols)
        for level in range(levels):
            piece = placed[:, level * LANES : (level + 1) * LANES]
            slab[here, level * capacity : (level + 1) * capacity, :] = piece.reshape(
                cols, capacity, LANES
            )

    pl.when(valid(0))(functools.partial(fill, 0))
    pl.when(band == 0)(functools.partial(fill, 2))

    inner_band = (band > 0) & (band < bands - 1)
    neighbours = jnp.where(inner_band, 2, 1) if bands > 1 else 0
    pl.semaphore_wait(barrier, half_size * (1 + neighbours))

    def send_to_half(source_of, target, sems_out, sems_in, offset):
        def one(step, carry):
            to = lax.rem(place_in_half + half_size // 2 + step, half_size)

            def start_remote():
                pltpu.make_async_remote_copy(
                    src_ref=source_of(to),
                    dst_ref=target,
                    send_sem=sems_out.at[offset],
                    recv_sem=sems_in.at[2 - offset],
                    device_id=(band + (offset - 1), half * half_size + to),
                    device_id_type=MESH,
                ).start()

            if offset == 1:
                pl.when(to != place_in_half)(start_remote)
            else:
                start_remote()
            return carry

        lax.fori_loop(0, half_size, one, 0, unroll=half_size <= 4)
        if offset == 1:
            pltpu.make_async_copy(source_of(place_in_half), target, sems_in.at[1]).start()

    def push_tags(offset):
        send_to_half(
            lambda to: tags_out.at[offset * half_size + to],
            tags_in.at[(2 - offset) * half_size + place_in_half],
            tag_send, tag_recv, offset,
        )

    def push(owner_half, owner_of, into, sems, offset):
        send_to_half(
            lambda to: slab.at[offset * cols + owner_half * half_size + owner_of(to)],
            into.at[(2 - offset) * half_size + place_in_half],
            send_sem, sems, offset,
        )

    cut_copy = pltpu.make_async_remote_copy(
        src_ref=cut_out,
        dst_ref=cut_in,
        send_sem=cut_send,
        recv_sem=cut_recv,
        device_id=counterpart,
        device_id_type=MESH,
    )

    def place_and_push(offset):
        if offset == 1:
            fill(offset)
        elif offset == 2:
            pl.when(band > 0)(functools.partial(fill, offset))
        push(1 - half, mirror, relay, relay_sem, offset)

    pl.when(valid(0))(functools.partial(place_and_push, 0))
    pl.when(band == 0)(functools.partial(place_and_push, 2))
    for offset in (0, 2, 1):
        pl.when(valid(offset))(functools.partial(push_tags, offset))
    cut_copy.start()
    pl.when((band > 0) & valid(2))(functools.partial(place_and_push, 2))
    place_and_push(1)
    for offset in (0, 2, 1):
        pl.when(valid(offset))(functools.partial(push, half, lambda to: to, recv, recv_sem, offset))

    for copy in operand_copies[5:]:
        copy.wait()
    begin = start[col]
    cos_start, sin_start = begin[0:1], begin[1:2]
    rotated[0] = fine[0] * cos_start - fine[1] * sin_start
    rotated[1] = fine[1] * cos_start + fine[0] * sin_start

    def table_step(step, carry):
        pair = coarse[step]
        cos_base, sin_base = pair[0:1], pair[1:2]
        cos_fine, sin_fine = rotated[0], rotated[1]
        at = pl.ds(pl.multiple_of(step * STEP, STEP), STEP)
        for first, value in (
            (0, cos_base * cos_fine - sin_base * sin_fine),
            (wave_count, sin_base * cos_fine + cos_base * sin_fine),
        ):
            high, low = split(value)
            table_high[at, first : first + wave_count] = high
            table_low[at, first : first + wave_count] = low
        return carry

    lax.fori_loop(0, coarse.shape[0], table_step, 0)

    tiles = sums.shape[1]
    sums[...] = jnp.zeros_like(sums)
    relay_sums[...] = jnp.zeros_like(relay_sums)

    def wait_tags(offset):
        here = tags_in.at[pl.ds(offset * half_size, half_size)]
        pltpu.make_async_copy(here, here, tag_recv.at[offset]).wait()

    for offset in (0, 2, 1):
        pl.when(valid(offset))(functools.partial(wait_tags, offset))

    def receive(ref, sems, into, kind, offset):
        here = pl.ds(offset * half_size, half_size)
        tag_rows = [
            tags_in[offset * half_size + sender, kind : kind + 1] for sender in range(half_size)
        ]
        tags = jnp.transpose(jnp.concatenate(tag_rows * (-(-8 // half_size)), axis=0))
        wide = lax.broadcasted_iota(jnp.int32, (capacity, tiles), 1).astype(F32)
        chooser = jnp.concatenate(
            [
                (tags[:capacity, sender : sender + 1] == wide).astype(F32)
                for sender in range(half_size)
            ],
            axis=0,
        )
        chooser = jnp.transpose(chooser).astype(BF16)
        pltpu.make_async_copy(ref.at[here], ref.at[here], sems.at[offset]).wait()
        incoming = jnp.concatenate(
            [
                ref[here, level * capacity : (level + 1) * capacity, :].reshape(
                    half_size * capacity, LANES
                )
                for level in range(levels)
            ],
            axis=1,
        )
        high, low = split(incoming)
        total = dot(chooser, high) + dot(chooser, low)
        for level in range(levels):
            into[level] += total[:, level * LANES : (level + 1) * LANES]

    def dense_start(first, count):
        here = (pl.ds(first, count), pl.ds(0, tile_count))
        pltpu.make_async_remote_copy(
            src_ref=relay_sums.at[here],
            dst_ref=passed.at[pl.ds(first, count)],
            send_sem=pass_send,
            recv_sem=pass_recv,
            device_id=counterpart,
            device_id_type=MESH,
        ).start()

    inner = jnp.where(half == 0, layer >= layers // 2, layer < layers - layers // 2)
    outer = jnp.logical_not(inner)
    ends = [levels * share // DENSE[-1] for share in DENSE]

    def dense_part(index):
        if ends[index + 1] > ends[index]:
            pl.when(outer)(
                functools.partial(dense_start, ends[index], ends[index + 1] - ends[index])
            )

    for offset in (0, 2, 1):
        pl.when(valid(offset))(functools.partial(receive, relay, relay_sem, relay_sums, 1, offset))
    pl.when(inner)(functools.partial(dense_start, 0, levels))
    dense_part(0)

    long_tiles, field_rows = field.shape[1:3]
    lat_band = field_rows // levels
    group_rows = field_rows // half_size
    shape3 = (levels, long_tiles, LANES)
    lane3 = lax.broadcasted_iota(jnp.int32, shape3, 2)
    inside = lax.broadcasted_iota(jnp.int32, shape3, 1) * LANES + lane3 < longitudes

    def row_of(level, lat):
        owner, within = divmod(lat, lat_here)
        lat_half, owner_place = divmod(owner, half_size)
        group = mirror(owner_place) if lat_half else owner_place
        return group * group_rows + (level * 2 + lat_half) * lat_here + within

    def lat_rows(ref, lat):
        first, shift = divmod(lat * longitudes, LANES)
        value = ref[:, first : first + long_tiles, :]
        if shift:
            after = ref[:, first + 1 : first + 1 + long_tiles, :]
            value = jnp.where(
                lane3 < LANES - shift,
                pltpu.roll(value, LANES - shift, 2),
                pltpu.roll(after, LANES - shift, 2),
            )
        return jnp.where(inside, value, 0.0)

    def rows_of_field(ref, index):
        for lat in range(lat_band):
            value = lat_rows(ref, lat)
            for level in range(levels):
                field[index, :, row_of(level, lat), :] = value[level]
        rows_wide = jnp.concatenate([field[index, tile] for tile in range(long_tiles)], axis=1)
        high, low = split(rows_wide)
        return jnp.concatenate([high, low], axis=0), high

    def transformed(parts, waves):
        both = dot(parts[0], table_high[:, waves])
        return both[:field_rows] + both[field_rows:] + dot(parts[1], table_low[:, waves])

    relayed = transformed(rows_of_field(relay_sums, 1), slice(None))
    angle = turn[col]
    cos_part, sin_part = relayed[:, :wave_count], relayed[:, wave_count:]
    grouped = (half_size, group_rows, wave_count)
    spectra[:, :, :wave_count] = (cos_part * angle[0:1] - sin_part * angle[1:2]).reshape(grouped)
    spectra[:, :, wave_count:] = (sin_part * angle[0:1] + cos_part * angle[1:2]).reshape(grouped)

    for offset in (0, 2, 1):
        pl.when(valid(offset))(functools.partial(receive, recv, recv_sem, sums, 0, offset))

    waves = 2 * wave_count
    pieces = [slice(first, first + PIECE) for first in range(0, waves, PIECE)]

    def to_half(source_of, target, sem_out, sem_in):
        def one(step, carry):
            to = lax.rem(place_in_half + half_size // 2 + step, half_size)

            def start_remote():
                pltpu.make_async_remote_copy(
                    src_ref=source_of(to),
                    dst_ref=target,
                    send_sem=sem_out,
                    recv_sem=sem_in,
                    device_id=(band, half * half_size + to),
                    device_id_type=MESH,
                ).start()

            pl.when(to != place_in_half)(start_remote)
            return carry

        lax.fori_loop(0, half_size, one, 0, unroll=half_size <= 4)
        pltpu.make_async_copy(source_of(place_in_half), target, sem_in).start()

    parts = rows_of_field(sums, 0)
    for i, piece in enumerate(pieces):
        if i % TOGETHER == 0:
            wide = slice(piece.start, piece.start + TOGETHER * PIECE)
            spectra[:, :, wide] += transformed(parts, wide).reshape(
                half_size, group_rows, TOGETHER * PIECE
            )
        to_half(
            lambda to: spectra.at[group_of(to), :, piece],
            arrived.at[place_in_half, :, piece],
            scatter_send.at[i], scatter_recv.at[i],
        )
    dense_part(1)

    cut_copy.wait()
    cuts = []
    for lat_half in range(2):
        for lat in range(lat_here):
            cuts.append(
                jnp.where(half == lat_half, cut_out[lat : lat + 1], cut_in[lat : lat + 1])
            )
    cut_rows = jnp.concatenate(cuts * (group_rows // len(cuts)), axis=0)

    def gain_of(tile):
        j = lax.broadcasted_iota(jnp.int32, (group_rows, LANES), 1) + tile * LANES
        wave = jnp.where(j >= wave_count, j - wave_count, j)
        weight = jnp.where(wave == 0, 1.0, 2.0) / period
        return jnp.where(wave <= cut_rows, weight, 0.0).astype(F32)

    gains = jnp.concatenate([gain_of(tile) for tile in range(waves // LANES)], axis=1)

    def cross(i):
        return pltpu.make_async_remote_copy(
            src_ref=half_sum.at[:, pieces[i]],
            dst_ref=other_sum.at[:, pieces[i]],
            send_sem=cross_send.at[i],
            recv_sem=cross_recv.at[i],
            device_id=counterpart,
            device_id_type=MESH,
        )

    for i, piece in enumerate(pieces):
        here = arrived.at[:, :, piece]
        pltpu.make_async_copy(here, here, scatter_recv.at[i]).wait()
        total = arrived[0, :, piece]
        for sender in range(1, half_size):
            total += arrived[sender, :, piece]
        half_sum[:, piece] = total
        cross(i).start()
    dense_part(2)
    for i, piece in enumerate(pieces):
        cross(i).wait_recv()
        scaled[:, piece] = (half_sum[:, piece] + other_sum[:, piece]) * gains[:, piece]
        to_half(
            lambda to: scaled.at[:, piece],
            gathered.at[group_of(place_in_half), :, piece],
            spread_send.at[i], spread_recv.at[i],
        )
        if i == BETWEEN:
            dense_part(3)
    dense_part(4)

    def drain(offset):
        sent = slab.at[pl.ds(0, cols - 2 if offset == 1 else cols)]
        pltpu.make_async_copy(sent, sent, send_sem.at[offset]).wait()
        tag = tags_out.at[pl.ds(0, half_size - 1 if offset == 1 else half_size)]
        pltpu.make_async_copy(tag, tag, tag_send.at[offset]).wait()

    for offset in range(3):
        pl.when(valid(offset))(functools.partial(drain, offset))
    for i, piece in enumerate(pieces):
        others = arrived.at[pl.ds(0, half_size - 1), :, piece]
        pltpu.make_async_copy(others, others, scatter_send.at[i]).wait()
        cross(i).wait_send()

    def natural(spread):
        rows_of = [
            spread[row : row + lat_here]
            for level in range(levels)
            for row in (row_of(level, lat) for lat in range(0, lat_band, lat_here))
        ]
        return jnp.concatenate(rows_of, axis=0)[:, :longitudes].reshape(
            levels, lat_band, longitudes
        )

    result = None
    for i, piece in enumerate(pieces):
        here = gathered.at[:, :, piece]
        pltpu.make_async_copy(here, here, spread_recv.at[i]).wait()
        high, low = split(gathered[:, :, piece].reshape(field_rows, PIECE))
        both = dot(jnp.concatenate([high, low], axis=0), table_high[:, piece], 1, 1)
        added = both[:field_rows] + both[field_rows:] + dot(high, table_low[:, piece], 1, 1)
        result = added if result is None else result + added
    filtered[...] = natural(result)

    pltpu.make_async_copy(passed, passed, pass_recv).wait()
    sums[:, :tile_count, :] += passed[...]
    for lat in range(lat_band):
        value = lat_rows(sums, lat)
        for level in range(levels):
            field[0, :, level * lat_band + lat, :] = value[level]
    rows_wide = jnp.concatenate([field[0, tile] for tile in range(long_tiles)], axis=1)
    remapped[...] = rows_wide[:, :longitudes].reshape(levels, lat_band, longitudes)

    pltpu.make_async_copy(passed, passed, pass_send).wait()
    for i, piece in enumerate(pieces):
        others = arrived.at[pl.ds(0, half_size - 1), :, piece]
        pltpu.make_async_copy(others, others, spread_send.at[i]).wait()


def deliver(first, second, first_out, second_out, sem):
    copies = [
        pltpu.make_async_copy(first, first_out, sem.at[0]),
        pltpu.make_async_copy(second, second_out, sem.at[1]),
    ]
    for copy in copies:
        copy.start()
    for copy in copies:
        copy.wait()


def cos_sin(positions):
    phases = positions[:, None] * np.arange(KW)[None, :] % NLON
    angles = phases * (2 * np.pi / NLON)
    return np.cos(angles).astype(np.float32), np.sin(angles).astype(np.float32)


def width_of(mesh):
    cols = mesh.shape["col"]
    places = [getattr(device, "coords", None) for device in mesh.devices[0]]
    if None in places:
        return 1
    width = sum(place[2] == places[0][2] for place in places)
    return width if cols % (2 * width) == 0 else 1


def local(mesh, source, weights, source_block, owner_device, target_tile, cutoff):
    bands, cols = mesh.shape["band"], mesh.shape["col"]
    levels = source.shape[0]
    block_count, block_width = weights.shape[:2]
    lat_here = cutoff.shape[0]
    lat_band = lat_here * cols
    half_size = cols // 2
    longitudes = NLON // cols
    cell_count = lat_band * longitudes
    tile_count = (cell_count + block_width - 1) // block_width
    regular = (tile_count + cols - 1) // cols
    capacity = regular + max(1, (block_count - cols * regular + 2 * cols - 1) // (2 * cols))
    capacity = round_up(capacity, 8)
    long_pad = round_up(longitudes, LANES)
    long_tiles = long_pad // LANES
    tiles = round_up(tile_count + long_tiles, LANES)
    sent_tiles = tile_count
    group_rows = levels * lat_band // half_size
    pieces = 2 * KW // PIECE
    chunks = block_count // CHUNK
    fine = np.stack(cos_sin(np.arange(STEP)))
    coarse = np.stack(cos_sin(STEP * np.arange(long_pad // STEP)), axis=1)
    start = np.stack(cos_sin(longitudes * np.arange(cols)), axis=1)
    width = width_of(mesh)
    places = np.arange(half_size)
    mirrored = (half_size // width - 1 - places // width) * width + places % width
    away = np.concatenate([half_size + mirrored - places, mirrored - places - half_size])
    turn = np.stack(cos_sin(longitudes * away % NLON), axis=1)

    slab_rows = levels * capacity
    vmem = pl.BlockSpec(memory_space=pltpu.VMEM)
    anywhere = pl.BlockSpec(memory_space=pl.ANY)
    shape = jax.ShapeDtypeStruct((levels, lat_band, longitudes), F32)
    dma = pltpu.SemaphoreType.DMA
    results = pl.pallas_call(
        functools.partial(
            remap_kernel, bands, cols, width, levels, capacity, KW, NLON, longitudes, sent_tiles
        ),
        out_shape=(pltpu.VMEM(shape.shape, F32), pltpu.VMEM(shape.shape, F32)),
        in_specs=[anywhere] * 10,
        out_specs=(vmem, vmem),
        scratch_shapes=[
            pltpu.SMEM(cutoff.shape, jnp.int32),
            pltpu.SMEM(source_block.shape, jnp.int32),
            pltpu.VMEM((1, block_count), jnp.int32),
            pltpu.VMEM((1, block_count), jnp.int32),
            pltpu.VMEM(source.shape, BF16),
            pltpu.VMEM(fine.shape, F32),
            pltpu.VMEM(coarse.shape, F32),
            pltpu.VMEM(start.shape, F32),
            pltpu.VMEM(turn.shape, F32),
            pltpu.VMEM(weights.shape, BF16),
            pltpu.VMEM((source.shape[1] // LANES, 16, LANES), BF16),
            pltpu.VMEM((source.shape[1] // LANES, 16, LANES), BF16),
            pltpu.VMEM((block_count, 8, LANES), F32),
            pltpu.VMEM((2 * block_count, levels * LANES), BF16),
            pltpu.VMEM((levels, tiles, LANES), F32),
            pltpu.VMEM((long_pad, 2 * KW), BF16),
            pltpu.VMEM((long_pad, 2 * KW), BF16),
            pltpu.VMEM((2, STEP, KW), F32),
            pltpu.VMEM((2, long_tiles, levels * lat_band, LANES), F32),
            pltpu.VMEM((3 * cols, slab_rows, LANES), F32),
            pltpu.VMEM((3 * half_size, slab_rows, LANES), F32),
            pltpu.VMEM((3 * half_size, slab_rows, LANES), F32),
            pltpu.VMEM((levels, tiles, LANES), F32),
            pltpu.VMEM((levels, sent_tiles, LANES), F32),
            pltpu.VMEM((3 * half_size, 2, LANES), F32),
            pltpu.VMEM((3 * half_size, 2, LANES), F32),
            pltpu.VMEM((lat_here, LANES), jnp.int32),
            pltpu.VMEM((lat_here, LANES), jnp.int32),
            pltpu.VMEM((half_size, group_rows, 2 * KW), F32),
            pltpu.VMEM((half_size, group_rows, 2 * KW), F32),
            pltpu.VMEM((group_rows, 2 * KW), F32),
            pltpu.VMEM((group_rows, 2 * KW), F32),
            pltpu.VMEM((group_rows, 2 * KW), F32),
            pltpu.VMEM((half_size, group_rows, 2 * KW), F32),
            dma((chunks,)),
            dma((3,)),
            dma((3,)),
            dma,
            dma,
            dma((3,)),
            dma((3,)),
            dma((3,)),
            dma,
            dma,
            dma((pieces,)),
            dma((pieces,)),
            dma((pieces,)),
            dma((pieces,)),
            dma((pieces,)),
            dma((pieces,)),
            dma((9,)),
        ],
        compiler_params=pltpu.CompilerParams(
            collective_id=0, has_side_effects=True, vmem_limit_bytes=48 << 20
        ),
    )(
        *(
            pltpu.with_memory_space_constraint(operand, pltpu.HBM)
            for operand in (
                cutoff,
                source_block,
                owner_device.reshape(1, block_count),
                target_tile.reshape(1, block_count),
                source,
                jnp.asarray(fine),
                jnp.asarray(coarse),
                jnp.asarray(start),
                jnp.asarray(turn),
                weights,
            )
        )
    )
    return pl.pallas_call(
        deliver,
        out_shape=(shape, shape),
        in_specs=[vmem] * 2,
        out_specs=(anywhere, anywhere),
        scratch_shapes=[dma((2,))],
    )(*(pltpu.with_memory_space_constraint(result, pltpu.VMEM) for result in results))


def solution(mesh):
    in_specs = (
        P(None, ("band", "col")),
        P(("band", "col"), None, None),
        P(("band", "col")),
        P(("band", "col"), None),
        P(("band", "col")),
        P(("band", "col")),
    )
    out_specs = (P(None, "band", "col"), P(None, "band", "col"))
    return jax.shard_map(
        functools.partial(local, mesh),
        mesh=mesh,
        in_specs=in_specs,
        out_specs=out_specs,
        check_vma=False,
    )
```
